512 devices in a mesh: gx: 16 (over z_lo, x), gy: 8 (over y, core), gz: 4 (over z_hi).
Axes of the slice: x: 4, y: 4, z: 16 (z_hi: 4, z_lo: 4; z = z_hi * 4 + z_lo), core: 2. Of those that a mesh axis runs over, the one named last changes fastest.
Arguments:
- populations: float32 [2, 19, 64, 128, 512], P(None, None, 'gx', 'gy', 'gz'), may hold values from 0.01 to 0.2
- solid: int32 [64, 128, 512], P('gx', 'gy', 'gz'), may hold values 0 or 1
Outputs:
- read: float32 [2, 19, 64, 128, 512], P(None, None, 'gx', 'gy', 'gz')
The draws below stay inside these ranges and needn't reach their ends.
All inputs are finite; a program needn't handle non-finite values. No bound on the sum of `solid` on one device may be relied on, other than what follows from the above.
Results may differ from the reference program's by a relative error of at most 0.0001.
Values sent between devices are 32-bit elements; how exact they have to be, the bound alone decides.
A program may use at most 64 MiB of HBM per device.

```python
import math
import jax
import jax.numpy as jnp
import numpy as np
from jax import lax

NX = 64
NY = 128
NZ = 512


def touch_ends(values, own_key, smallest, high):
    extent = values.shape
    index_at = [jax.random.randint(jax.random.fold_in(own_key, axis), (), 0, extent[axis]) for axis in range(len(extent))]
    values = values.at[tuple(index_at)].set(smallest)
    longest = extent.index(max(extent))
    index_at[longest] = (index_at[longest] + 1) % extent[longest]
    return values.at[tuple(index_at)].set(high)


def steps_of(own_key, extent, shards, least, top_value):
    factor_of, own = 1.0, jax.random.fold_in(own_key, 6)
    for dim, blocks in shards:
        steps = jnp.exp(jax.random.uniform(jax.random.fold_in(own, dim), (blocks,), jnp.float32, least / len(shards), top_value / len(shards)))
        factor_of = factor_of * jnp.repeat(steps, extent[dim] // blocks).reshape([-1 if axis == dim else 1 for axis in range(len(extent))])
    return factor_of


def setup_inputs(seed: int = 0) -> dict:
    key_of = jax.random.split(jax.random.key(seed), 3)
    return {
        "populations": jnp.clip(jnp.exp(math.log(0.2) - 2.9957323 * jax.random.uniform(key_of[0], (2, 19, NX, NY, NZ), jnp.float32) ** steps_of(key_of[0], (2, 19, NX, NY, NZ), ((2, 16), (3, 8), (4, 4)), -0.2, 0.2)), 0.01, 0.2),
        "solid": touch_ends((jax.random.randint(key_of[1], (NX, NY, NZ), 0, 8) < 1).astype(jnp.int32), jax.random.fold_in(key_of[1], 1), 0, 1),
    }


VELOCITIES = [(0, 0, 0), (1, 0, 0), (-1, 0, 0), (0, 1, 0), (0, -1, 0), (0, 0, 1), (0, 0, -1),
              (1, 1, 0), (-1, -1, 0), (1, -1, 0), (-1, 1, 0), (1, 0, 1), (-1, 0, -1), (1, 0, -1),
              (-1, 0, 1), (0, 1, 1), (0, -1, -1), (0, 1, -1), (0, -1, 1)]
WEIGHTS = [1.0 / 3.0] + [1.0 / 18.0] * 6 + [1.0 / 36.0] * 12
OPPOSITE = [0, 2, 1, 4, 3, 6, 5, 8, 7, 10, 9, 12, 11, 14, 13, 16, 15, 18, 17]
coupling = 0.9
relax_times = (1.0, 0.8)
wall_values = (0.3, 1.5)


def collide(populations, fluid, psi, gradient):
    vel = jnp.asarray(np.array(VELOCITIES, np.float32))
    weights = jnp.asarray(np.array(WEIGHTS, np.float32))
    rho = jnp.sum(populations, axis=1)
    moment = jnp.einsum("ia,kixyz->kaxyz", vel, populations, precision=lax.Precision.HIGHEST)
    inv_first = 1.0 / relax_times[0]
    inv_second = 1.0 / relax_times[1]
    weight_sum = rho[0] * inv_first + rho[1] * inv_second
    common = (moment[0] * inv_first + moment[1] * inv_second) / weight_sum[None]
    forces = (-coupling * psi[0][None] * gradient[1], -coupling * psi[1][None] * gradient[0])
    results = []
    for comp in range(2):
        velocity = common + relax_times[comp] * forces[comp] / rho[comp][None]
        along = jnp.einsum("ia,axyz->ixyz", vel, velocity, precision=lax.Precision.HIGHEST)
        speed_sq = jnp.sum(velocity * velocity, axis=0)
        equil = weights[:, None, None, None] * rho[comp][None] * (
            1.0 + 3.0 * along + 4.5 * along * along - 1.5 * speed_sq[None])
        current = populations[comp]
        results.append(current - (current - equil) / relax_times[comp])
    post = jnp.stack(results, axis=0)
    return jnp.where(fluid[None, None], post, populations)


def reference(populations, solid):
    fluid = solid == 0
    rho = jnp.sum(populations, axis=1)
    wall = jnp.asarray(np.array(wall_values, np.float32)).reshape(2, 1, 1, 1)
    psi = jnp.where(fluid[None], rho, wall)
    parts = [jnp.zeros_like(psi) for axis_idx in range(3)]
    for i in range(1, 19):
        move = VELOCITIES[i]
        shifted = jnp.roll(psi, (-move[0], -move[1], -move[2]), axis=(1, 2, 3))
        for axis_idx in range(3):
            if move[axis_idx] != 0:
                parts[axis_idx] = parts[axis_idx] + (WEIGHTS[i] * move[axis_idx]) * shifted
    gradient = jnp.stack(parts, axis=1)
    post = collide(populations, fluid, psi, gradient)
    moved = []
    for i in range(19):
        move = VELOCITIES[i]
        pulled = jnp.roll(post[:, i], move, axis=(1, 2, 3))
        source_fluid = jnp.roll(fluid, move, axis=(0, 1, 2))
        moved.append(jnp.where(source_fluid[None], pulled, post[:, OPPOSITE[i]]))
    result = jnp.stack(moved, axis=1)
    return jnp.where(fluid[None, None], result, populations)
```

```python
import functools

import jax
import jax.numpy as jnp
from jax import lax
from jax.experimental import pallas as pl
from jax.experimental.pallas import tpu as pltpu
from jax.sharding import PartitionSpec as P

VELOCITIES = [
    (0, 0, 0),
    (1, 0, 0),
    (-1, 0, 0),
    (0, 1, 0),
    (0, -1, 0),
    (0, 0, 1),
    (0, 0, -1),
    (1, 1, 0),
    (-1, -1, 0),
    (1, -1, 0),
    (-1, 1, 0),
    (1, 0, 1),
    (-1, 0, -1),
    (1, 0, -1),
    (-1, 0, 1),
    (0, 1, 1),
    (0, -1, -1),
    (0, 1, -1),
    (0, -1, 1),
]
WEIGHTS = [1.0 / 3.0] + [1.0 / 18.0] * 6 + [1.0 / 36.0] * 12
OPPOSITE = [0, 2, 1, 4, 3, 6, 5, 8, 7, 10, 9, 12, 11, 14, 13, 16, 15, 18, 17]
PAIRS = [(1, 2), (3, 4), (5, 6), (7, 8), (9, 10), (11, 12), (13, 14), (15, 16), (17, 18)]
coupling = 0.9
relax_times = (1.0, 0.8)
wall_values = (0.3, 1.5)

NX_L, NY_L, NZ_L = 4, 16, 128
ROWS = 24
X_DIRS = ([i for i in range(19) if VELOCITIES[i][0] == 1], [i for i in range(19) if VELOCITIES[i][0] == -1])
Y_DIRS = ([i for i in range(19) if VELOCITIES[i][1] == 1], [i for i in range(19) if VELOCITIES[i][1] == -1])
Z_LOW = [i for i in range(19) if VELOCITIES[i][2] == 1]
Z_HIGH = [OPPOSITE[i] for i in Z_LOW]
BIG = 1e30
LIMIT = 1e28
FACE, DIAG = 1.0 / 18.0, 1.0 / 36.0
MESH = pl.DeviceIdType.MESH


def roll(a, shift, axis):
    return pltpu.roll(a, shift % a.shape[axis], axis)


def posts(k, fluid, rho, v, dirs, old):
    scale = 1.0 / relax_times[k]
    r = jnp.where(fluid, rho * scale, 0.0)
    b = [1.5 * c for c in v]
    quad = b[0] * b[0] + b[1] * b[1] + b[2] * b[2]
    base = r - (2.0 / 3.0) * r * quad
    base = jnp.where(fluid, base, BIG)
    out = {}

    def keep(i, eq):
        out[i] = eq if k == 0 else eq + (1.0 - scale) * old(i)

    if 0 in dirs:
        keep(0, WEIGHTS[0] * base)
    by_weight = {}
    for pair in PAIRS:
        if not any(i in dirs for i in pair):
            continue
        i = pair[0]
        w = WEIGHTS[i]
        if w not in by_weight:
            by_weight[w] = (w * base, (2.0 * w) * r)
        wb, wr = by_weight[w]
        along = None
        for axis in range(3):
            c = VELOCITIES[i][axis]
            if c:
                along = (b[axis] if c > 0 else -b[axis]) if along is None else (along + b[axis] if c > 0 else along - b[axis])
        t = wr * along
        s = wb + along * t
        if i in dirs:
            keep(i, s + t)
        if pair[1] in dirs:
            keep(pair[1], s - t)
    return out


def kernel(
    pop, solid, out, f0, f1, flag, sp, u, gq, gvp, gv, gwp, gw, post,
    ys, yr, xs, xr, xys, xyr, zs, zr, xzs, xzr, sem_in, send, recv,
):
    ix, iy, iz = lax.axis_index("gx"), lax.axis_index("gy"), lax.axis_index("gz")
    nx, ny, nz = lax.axis_size("gx"), lax.axis_size("gy"), lax.axis_size("gz")
    xd = ({"gx": lax.rem(ix + 1, nx)}, {"gx": lax.rem(ix + nx - 1, nx)})
    yd = ({"gy": lax.rem(iy + 1, ny)}, {"gy": lax.rem(iy + ny - 1, ny)})
    zd = ({"gz": lax.rem(iz + 1, nz)}, {"gz": lax.rem(iz + nz - 1, nz)})

    barrier = pltpu.get_barrier_semaphore()
    for target in (*zd, *xd, *yd):
        pl.semaphore_signal(barrier, inc=1, device_id=target, device_id_type=MESH)
    loads = [
        pltpu.make_async_copy(solid, flag, sem_in.at[0]),
        pltpu.make_async_copy(pop.at[0], f0, sem_in.at[1]),
        pltpu.make_async_copy(pop.at[1], f1.at[:, 1:5, 0:16, :], sem_in.at[2]),
    ]
    for copy in loads:
        copy.start()

    slots = iter(range(12))

    def remote(src, dst, target):
        n = next(slots)
        return pltpu.make_async_remote_copy(
            src_ref=src, dst_ref=dst, send_sem=send.at[n], recv_sem=recv.at[n], device_id=target, device_id_type=MESH
        )

    for copy in loads:
        copy.wait()

    for x in range(NX_L):
        fluid = flag[x] == 0
        rho, momentum = [], []
        for k in range(2):
            f = (lambda i: f0[i, x]) if k == 0 else (lambda i: f1[i, x + 1, 0:16, :])
            total = f(0)
            mom = [None, None, None]
            for i, j in PAIRS:
                a, b = f(i), f(j)
                total = total + (a + b)
                d = a - b
                for axis in range(3):
                    c = VELOCITIES[i][axis]
                    if c:
                        mom[axis] = d * float(c) if mom[axis] is None else (mom[axis] + d if c > 0 else mom[axis] - d)
            rho.append(total)
            momentum.append(mom)
            sp[k, x + 2, 0:16, :] = jnp.where(fluid, total, -wall_values[k])
        inv = 1.0 / (rho[0] * (1.0 / relax_times[0]) + rho[1] * (1.0 / relax_times[1]))
        for axis in range(3):
            u[axis, x + 1, 0:16, :] = (
                momentum[0][axis] * (1.0 / relax_times[0]) + momentum[1][axis] * (1.0 / relax_times[1])
            ) * inv

    for s in range(2):
        edge, two = ((15, 14), (0, 0))[s]
        for k in range(2):
            for x in range(NX_L):
                r = (k * 4 + x) * 2
                ys[s, r : r + 2, :] = sp[k, x + 2, two : two + 2, :]
        for axis in range(3):
            for x in range(NX_L):
                r = 16 + axis * 4 + x
                ys[s, r : r + 1, :] = u[axis, x + 1, edge : edge + 1, :]
        for j, i in enumerate(Y_DIRS[s]):
            for x in range(NX_L):
                r = 28 + j * 4 + x
                ys[s, r : r + 1, :] = f1[i, x + 1, edge : edge + 1, :]
        for k in range(2):
            for layer in range(2):
                xs[s, k * 2 + layer] = sp[k, 2 + (2 + layer if s == 0 else layer), 0:16, :]
        last = 4 if s == 0 else 1
        for axis in range(3):
            xs[s, 4 + axis] = u[axis, last, 0:16, :]
        for j, i in enumerate(X_DIRS[s]):
            xs[s, 7 + j] = f1[i, last, 0:16, :]

    pl.semaphore_wait(barrier, 6)
    y_copies = [remote(ys.at[s], yr.at[s], yd[s]) for s in range(2)]
    x_copies = [remote(xs.at[s], xr.at[s], xd[s]) for s in range(2)]
    for copy in (*y_copies, *x_copies):
        copy.start()

    lane = lax.broadcasted_iota(jnp.int32, (ROWS, NZ_L), 1)
    tail = lax.broadcasted_iota(jnp.int32, (8, NZ_L), 0)

    for copy in y_copies:
        copy.wait_recv()
    for s in range(2):
        edge, two = ((23, 22), (16, 16))[s]
        for k in range(2):
            for x in range(NX_L):
                r = (k * 4 + x) * 2
                sp[k, x + 2, two : two + 2, :] = yr[s, r : r + 2, :]
        for axis in range(3):
            for x in range(NX_L):
                r = 16 + axis * 4 + x
                u[axis, x + 1, edge : edge + 1, :] = yr[s, r : r + 1, :]
        for j, i in enumerate(Y_DIRS[s]):
            for x in range(NX_L):
                r = 28 + j * 4 + x
                f1[i, x + 1, edge : edge + 1, :] = yr[s, r : r + 1, :]

    for s in range(2):
        near, far = ((127, 126), (0, 1))[s]
        dirs = (Z_LOW, Z_HIGH)[s]
        tile = jnp.zeros((ROWS, NZ_L), jnp.float32)
        for v in range(12):
            for x in range(NX_L):
                if v < 4:
                    value, column = sp[v % 2, x + 2], near if v < 2 else far
                elif v < 7:
                    value, column = u[v - 4, x + 1], near
                else:
                    value, column = f1[dirs[v - 7], x + 1], near
                spot = v * 8 + x + 2
                tile = jnp.where(lane == spot, roll(value, spot - column, 1), tile)
        zs[s] = tile
    z_copies = [remote(zs.at[s], zr.at[s], zd[s]) for s in range(2)]
    for copy in z_copies:
        copy.start()
    for s in range(2):
        last = 4 if s == 0 else 1
        for k in range(2):
            for layer in range(2):
                xys[s, k * 2 + layer] = sp[k, 2 + (2 + layer if s == 0 else layer), 16:24, :]
        for axis in range(3):
            xys[s, 4 + axis] = u[axis, last, 16:24, :]
        up, down = ((7, 9), (10, 8))[s]
        xys[s, 7] = jnp.where(tail < 4, f1[down, last, 16:24, :], f1[up, last, 16:24, :])
    xy_copies = [remote(xys.at[s], xyr.at[s], xd[s]) for s in range(2)]
    own_copies = [remote(zs, xzs.at[s], xd[s]) for s in range(2)]
    for copy in (*xy_copies, *own_copies):
        copy.start()

    for copy in z_copies:
        copy.wait_recv()
    xz_copies = [remote(zr, xzr.at[s], xd[s]) for s in range(2)]
    for copy in xz_copies:
        copy.start()

    for copy in (*x_copies, *xy_copies):
        copy.wait_recv()
    for s in range(2):
        last = 0 if s == 0 else 5
        for k in range(2):
            for layer in range(2):
                plane = layer if s == 0 else 6 + layer
                sp[k, plane, 0:16, :] = xr[s, k * 2 + layer]
                sp[k, plane, 16:24, :] = xyr[s, k * 2 + layer]
        for axis in range(3):
            u[axis, last, 0:16, :] = xr[s, 4 + axis]
            u[axis, last, 16:24, :] = xyr[s, 4 + axis]
        for j, i in enumerate(X_DIRS[s]):
            f1[i, last, 0:16, :] = xr[s, 7 + j]
            if VELOCITIES[i][1]:
                f1[i, last, 16:24, :] = xyr[s, 7]

    for copy in (*own_copies, *xz_copies):
        copy.wait_recv()

    part = lane % 8

    def merged(own, low, high):
        return jnp.where(part < 2, roll(low, -4, 1), jnp.where(part > 5, roll(high, 4, 1), own))

    low = merged(zr[0], xzr[0, 0], xzr[1, 0])
    high = merged(zr[1], xzr[0, 1], xzr[1, 1])
    own_low = merged(zs[1], xzs[0, 1], xzs[1, 1])
    own_high = merged(zs[0], xzs[0, 0], xzs[1, 0])

    for k in range(2):
        for p in range(8):
            a = jnp.abs(sp[k, p])
            above = jnp.where(lane == 127, roll(jnp.abs(high), 127 - (k * 8 + p), 1), roll(a, -1, 1))
            below = jnp.where(lane == 0, roll(jnp.abs(low), -(k * 8 + p), 1), roll(a, 1, 1))
            pz, w = above + below, above - below
            a_up, a_down = roll(a, -1, 0), roll(a, 1, 0)
            gq[k, p] = FACE * a + DIAG * (a_up + a_down + pz)
            v = a_up - a_down
            gv[k, p] = DIAG * v
            gw[k, p] = DIAG * w
            if 1 <= p <= 6:
                gvp[k, p] = FACE * v + DIAG * (roll(pz, -1, 0) - roll(pz, 1, 0))
                gwp[k, p] = FACE * w + DIAG * (roll(w, -1, 0) + roll(w, 1, 0))

    for p in range(1, 7):
        grad = [
            (
                gq[k, p + 1] - gq[k, p - 1],
                gvp[k, p] + gv[k, p + 1] + gv[k, p - 1],
                gwp[k, p] + gw[k, p + 1] + gw[k, p - 1],
            )
            for k in range(2)
        ]
        dirs = X_DIRS[0] if p == 1 else X_DIRS[1] if p == 6 else list(range(19))
        for k in range(2):
            value = sp[k, p]
            vel = [u[axis, p - 1] - (coupling * relax_times[k]) * grad[1 - k][axis] for axis in range(3)]
            for i, item in posts(k, value > 0.0, value, vel, dirs, lambda i: f1[i, p - 1]).items():
                post[k, i, p - 1] = item

    def both(a, va, b, vb):
        return jnp.where(lane < 8, roll(a, -8 * va, 1), roll(b, 8 - 8 * vb, 1))

    value = [both(low, k, high, k) for k in range(2)]
    grad = []
    for k in range(2):
        a = jnp.abs(value[k])
        below = jnp.abs(both(low, 2 + k, own_high, k))
        above = jnp.abs(both(own_low, k, high, 2 + k))
        pz, w = above + below, above - below
        a_up, a_down = roll(a, -1, 0), roll(a, 1, 0)
        q = FACE * a + DIAG * (a_up + a_down + pz)
        v = a_up - a_down
        grad.append(
            (
                roll(q, -1, 1) - roll(q, 1, 1),
                FACE * v + DIAG * (roll(pz, -1, 0) - roll(pz, 1, 0) + roll(v, -1, 1) + roll(v, 1, 1)),
                FACE * w + DIAG * (roll(w, -1, 0) + roll(w, 1, 0) + roll(w, -1, 1) + roll(w, 1, 1)),
            )
        )
    sign = jnp.where(lane < 8, 1.0, -1.0)
    common = [both(low, 4 + axis, high, 4 + axis) for axis in range(3)]
    beyond = [
        posts(
            k,
            value[k] > 0.0,
            jnp.abs(value[k]),
            [sign * (common[axis] - (coupling * relax_times[k]) * grad[1 - k][axis]) for axis in range(3)],
            Z_LOW,
            lambda i: both(low, 7 + Z_LOW.index(i), high, 7 + Z_LOW.index(i)),
        )
        for k in range(2)
    ]

    lane16 = lax.broadcasted_iota(jnp.int32, (NY_L, NZ_L), 1)
    for k in range(2):
        for i in range(19):
            cx, cy, cz = VELOCITIES[i]
            if cz:
                side = beyond[k][i if cz > 0 else OPPOSITE[i]]
                side = (roll(side, cy, 0) if cy else side)[0:16]
            for x in range(NX_L):
                fluid = flag[x] == 0
                old = f0[i, x] if k == 0 else f1[i, x + 1, 0:16, :]
                if i == 0:
                    moved = post[k, 0, x + 1, 0:16, :]
                else:
                    moved = post[k, i, x + 1 - cx]
                    moved = (roll(moved, cy, 0) if cy else moved)[0:16]
                    if cz > 0:
                        moved = jnp.where(lane16 == 0, roll(side, -(x - cx + 2), 1), roll(moved, 1, 1))
                    elif cz < 0:
                        moved = jnp.where(lane16 == 127, roll(side, 127 - (x - cx + 10), 1), roll(moved, -1, 1))
                    moved = jnp.where(moved < LIMIT, moved, post[k, OPPOSITE[i], x + 1, 0:16, :])
                out[k, i, x] = jnp.where(fluid, moved, old)

    for copy in (*y_copies, *x_copies, *z_copies, *xy_copies, *own_copies, *xz_copies):
        copy.wait_send()


def body(populations, solid):
    f32 = jnp.float32
    plane = (ROWS, NZ_L)
    scratch = [
        pltpu.VMEM((19, 4, 16, 128), f32),
        pltpu.VMEM((19, 6, *plane), f32),
        pltpu.VMEM((4, 16, 128), jnp.int32),
        pltpu.VMEM((2, 8, *plane), f32),
        pltpu.VMEM((3, 6, *plane), f32),
        *[pltpu.VMEM((2, 8, *plane), f32)] * 5,
        pltpu.VMEM((2, 19, 6, *plane), f32),
        *[pltpu.VMEM((2, 48, 128), f32)] * 2,
        *[pltpu.VMEM((2, 12, 16, 128), f32)] * 2,
        *[pltpu.VMEM((2, 8, 8, 128), f32)] * 2,
        *[pltpu.VMEM((2, *plane), f32)] * 2,
        *[pltpu.VMEM((2, 2, *plane), f32)] * 2,
        pltpu.SemaphoreType.DMA((3,)),
        pltpu.SemaphoreType.DMA((12,)),
        pltpu.SemaphoreType.DMA((12,)),
    ]
    return pl.pallas_call(
        kernel,
        out_shape=jax.ShapeDtypeStruct(populations.shape, f32),
        in_specs=[pl.BlockSpec(memory_space=pl.ANY)] * 2,
        out_specs=pl.BlockSpec(memory_space=pltpu.VMEM),
        scratch_shapes=scratch,
        compiler_params=pltpu.CompilerParams(
            collective_id=0, has_side_effects=True, vmem_limit_bytes=40 * 1024 * 1024
        ),
    )(populations, solid)


def solution(mesh):
    in_specs = (P(None, None, "gx", "gy", "gz"), P("gx", "gy", "gz"))
    out_specs = P(None, None, "gx", "gy", "gz")
    return jax.shard_map(body, mesh=mesh, in_specs=in_specs, out_specs=out_specs, check_vma=False)
```

```python
import functools

import jax
import jax.numpy as jnp
from jax import lax
from jax.experimental import pallas as pl
from jax.experimental.pallas import tpu as pltpu
from jax.sharding import PartitionSpec as P

VELOCITIES = [
    (0, 0, 0),
    (1, 0, 0),
    (-1, 0, 0),
    (0, 1, 0),
    (0, -1, 0),
    (0, 0, 1),
    (0, 0, -1),
    (1, 1, 0),
    (-1, -1, 0),
    (1, -1, 0),
    (-1, 1, 0),
    (1, 0, 1),
    (-1, 0, -1),
    (1, 0, -1),
    (-1, 0, 1),
    (0, 1, 1),
    (0, -1, -1),
    (0, 1, -1),
    (0, -1, 1),
]
WEIGHTS = [1.0 / 3.0] + [1.0 / 18.0] * 6 + [1.0 / 36.0] * 12
OPPOSITE = [0, 2, 1, 4, 3, 6, 5, 8, 7, 10, 9, 12, 11, 14, 13, 16, 15, 18, 17]
PAIRS = [(1, 2), (3, 4), (5, 6), (7, 8), (9, 10), (11, 12), (13, 14), (15, 16), (17, 18)]
coupling = 0.9
relax_times = (1.0, 0.8)
wall_values = (0.3, 1.5)

NX_L, NY_L, NZ_L = 4, 16, 128
ROWS = 24
X_DIRS = ([i for i in range(19) if VELOCITIES[i][0] == 1], [i for i in range(19) if VELOCITIES[i][0] == -1])
Y_DIRS = ([i for i in range(19) if VELOCITIES[i][1] == 1], [i for i in range(19) if VELOCITIES[i][1] == -1])
Z_LOW = [i for i in range(19) if VELOCITIES[i][2] == 1]
Z_HIGH = [OPPOSITE[i] for i in Z_LOW]
BIG = 1e30
LIMIT = 1e28
FACE, DIAG = 1.0 / 18.0, 1.0 / 36.0
MESH = pl.DeviceIdType.MESH


def roll(a, shift, axis):
    return pltpu.roll(a, shift % a.shape[axis], axis)


def posts(k, fluid, rho, v, dirs, old):
    scale = 1.0 / relax_times[k]
    r = jnp.where(fluid, rho * scale, 0.0)
    b = [1.5 * c for c in v]
    quad = b[0] * b[0] + b[1] * b[1] + b[2] * b[2]
    base = r - (2.0 / 3.0) * r * quad
    base = jnp.where(fluid, base, BIG)
    out = {}

    def keep(i, eq):
        out[i] = eq if k == 0 else eq + (1.0 - scale) * old(i)

    if 0 in dirs:
        keep(0, WEIGHTS[0] * base)
    by_weight = {}
    for pair in PAIRS:
        if not any(i in dirs for i in pair):
            continue
        i = pair[0]
        w = WEIGHTS[i]
        if w not in by_weight:
            by_weight[w] = (w * base, (2.0 * w) * r)
        wb, wr = by_weight[w]
        along = None
        for axis in range(3):
            c = VELOCITIES[i][axis]
            if c:
                along = (b[axis] if c > 0 else -b[axis]) if along is None else (along + b[axis] if c > 0 else along - b[axis])
        t = wr * along
        s = wb + along * t
        if i in dirs:
            keep(i, s + t)
        if pair[1] in dirs:
            keep(pair[1], s - t)
    return out


def index_of(c):
    return 0 if c > 0 else 1


def ahead(ix, iz, nx, nz, dx, dz):
    if dz:
        rank = (lambda g: jnp.where(g < 2, g, 5 - g)) if nz == 4 else (lambda g: g)
        return rank(iz) > rank(lax.rem(iz + dz + nz, nz))
    if dx:
        return lax.rem(ix, 4) > lax.rem(lax.rem(ix + dx + nx, nx), 4)
    return None


def kernel(
    pop, flag, out, f0, f1, sp, u, gq, gvp, gv, gwp, gw, post,
    ys, yr, xs, xr, xys, xyr, tile, zs, zr, xzr, ps, yzr, xyzr, rest, sem_in, send, recv,
):
    ix, iy, iz = lax.axis_index("gx"), lax.axis_index("gy"), lax.axis_index("gz")
    nx, ny, nz = lax.axis_size("gx"), lax.axis_size("gy"), lax.axis_size("gz")
    around = (0, 1, -1)
    groups = [(dx, dz) for dz in (1, -1) for dx in around] + [(1, 0), (-1, 0)]
    sends_first = {g: ahead(ix, iz, nx, nz, *g) for g in groups}

    def target(dx, dy, dz):
        place = {}
        if dx:
            place["gx"] = lax.rem(ix + dx + nx, nx)
        if dy:
            place["gy"] = lax.rem(iy + dy + ny, ny)
        if dz:
            place["gz"] = lax.rem(iz + dz + nz, nz)
        return place

    loads = [
        pltpu.make_async_copy(pop.at[0], f0, sem_in.at[0]),
        pltpu.make_async_copy(pop.at[1], f1.at[:, 1:5, 0:16, :], sem_in.at[1]),
    ]
    for copy in loads:
        copy.start()
    barrier = pltpu.get_barrier_semaphore()
    count = 2
    for dx, dz in groups:
        first = sends_first[dx, dz]
        count = count + 3 * first.astype(jnp.int32)

        @pl.when(jnp.logical_not(first))
        def _(dx=dx, dz=dz):
            for dy in around:
                pl.semaphore_signal(barrier, inc=1, device_id=target(dx, dy, dz), device_id_type=MESH)

    for dy in (1, -1):
        pl.semaphore_signal(barrier, inc=1, device_id=target(0, dy, 0), device_id_type=MESH)

    ways = [(dx, dy, dz) for dz in around for dx in around for dy in around if dx or dy or dz]
    copies = {}
    for n, (dx, dy, dz) in enumerate(ways):
        x, y, z = index_of(dx), index_of(dy), index_of(dz)
        if dz:
            src = ps.at[z, y] if dy else zs.at[z]
            if dx:
                dst = xyzr.at[x, y, z] if dy else xzr.at[x, z]
            else:
                dst = yzr.at[y, z] if dy else zr.at[z]
        elif dx:
            src, dst = (xys.at[x, y], xyr.at[x, y]) if dy else (xs.at[x], xr.at[x])
        else:
            src, dst = ys.at[y], yr.at[y]
        copies[dx, dy, dz] = pltpu.make_async_remote_copy(
            src_ref=src, dst_ref=dst, send_sem=send.at[n], recv_sem=recv.at[n],
            device_id=target(dx, dy, dz), device_id_type=MESH,
        )

    for copy in loads:
        copy.wait()

    for x in range(NX_L):
        fluid = flag[x] == 0
        rho, momentum = [], []
        for k in range(2):
            f = (lambda i: f0[i, x]) if k == 0 else (lambda i: f1[i, x + 1, 0:16, :])
            total = f(0)
            mom = [None, None, None]
            for i, j in PAIRS:
                a, b = f(i), f(j)
                total = total + (a + b)
                d = a - b
                for axis in range(3):
                    c = VELOCITIES[i][axis]
                    if c:
                        mom[axis] = d * float(c) if mom[axis] is None else (mom[axis] + d if c > 0 else mom[axis] - d)
            rho.append(total)
            momentum.append(mom)
            sp[k, x + 2, 0:16, :] = jnp.where(fluid, total, -wall_values[k])
        inv = 1.0 / (rho[0] * (1.0 / relax_times[0]) + rho[1] * (1.0 / relax_times[1]))
        for axis in range(3):
            u[axis, x + 1, 0:16, :] = (
                momentum[0][axis] * (1.0 / relax_times[0]) + momentum[1][axis] * (1.0 / relax_times[1])
            ) * inv

    lane = lax.broadcasted_iota(jnp.int32, (ROWS, NZ_L), 1)
    lane16 = lax.broadcasted_iota(jnp.int32, (NY_L, NZ_L), 1)
    part = lax.broadcasted_iota(jnp.int32, (8, NZ_L), 1) % 8

    for s in range(2):
        near, far = ((127, 126), (0, 1))[s]
        dirs = (Z_LOW, Z_HIGH)[s]
        packed = jnp.zeros((NY_L, NZ_L), jnp.float32)
        for v in range(12):
            for x in range(NX_L):
                if v < 4:
                    value, column = sp[v % 2, x + 2, 0:16, :], near if v < 2 else far
                elif v < 7:
                    value, column = u[v - 4, x + 1, 0:16, :], near
                else:
                    value, column = f1[dirs[v - 7], x + 1, 0:16, :], near
                spot = v * 8 + x + 2
                packed = jnp.where(lane16 == spot, roll(value, spot - column, 1), packed)
        tile[s] = packed
        zs[s] = jnp.where((part >= 2) & (part <= 5), packed[0:8], roll(packed[8:16], 4, 1))
        ps[s, 0] = packed[14:16]
        ps[s, 1] = packed[0:2]

    def start_first(group):
        @pl.when(sends_first[group])
        def _():
            for dy in around:
                copies[group[0], dy, group[1]].start()

    def answer(group):
        @pl.when(jnp.logical_not(sends_first[group]))
        def _():
            for dy in around:
                copies[-group[0], -dy, -group[1]].wait_recv()
                copies[group[0], dy, group[1]].start()

    def collect(group):
        @pl.when(sends_first[group])
        def _():
            for dy in around:
                copies[-group[0], -dy, -group[1]].wait_recv()

    pl.semaphore_wait(barrier, count)
    for group in groups[:6]:
        start_first(group)

    for s in range(2):
        edge, two = ((15, 14), (0, 0))[s]
        for k in range(2):
            for x in range(NX_L):
                r = (k * 4 + x) * 2
                ys[s, r : r + 2, :] = sp[k, x + 2, two : two + 2, :]
        for axis in range(3):
            for x in range(NX_L):
                r = 16 + axis * 4 + x
                ys[s, r : r + 1, :] = u[axis, x + 1, edge : edge + 1, :]
        for j, i in enumerate(Y_DIRS[s]):
            for x in range(NX_L):
                r = 28 + j * 4 + x
                ys[s, r : r + 1, :] = f1[i, x + 1, edge : edge + 1, :]
        for side in range(2):
            ys[s, 48 + 2 * side : 50 + 2 * side, :] = tile[side, two : two + 2, :]
    for dy in (1, -1):
        copies[0, dy, 0].start()
    for s in range(2):
        last = 4 if s == 0 else 1
        planes = [(k, 2 + (2 + layer if s == 0 else layer)) for k in range(2) for layer in range(2)]
        for n, (k, plane) in enumerate(planes):
            xs[s, n] = sp[k, plane, 0:16, :]
        for axis in range(3):
            xs[s, 4 + axis] = u[axis, last, 0:16, :]
        for j, i in enumerate(X_DIRS[s]):
            xs[s, 7 + j] = f1[i, last, 0:16, :]
        for side in range(2):
            xs[s, 12 + side] = tile[side]
        for t in range(2):
            edge, two = ((15, 14), (0, 0))[t]
            for n, (k, plane) in enumerate(planes):
                xys[s, t, 2 * n : 2 * n + 2, :] = sp[k, plane, two : two + 2, :]
            for axis in range(3):
                xys[s, t, 8 + axis : 9 + axis, :] = u[axis, last, edge : edge + 1, :]
            i = VELOCITIES.index((1 - 2 * s, 1 - 2 * t, 0))
            xys[s, t, 11:12, :] = f1[i, last, edge : edge + 1, :]
            for side in range(2):
                xys[s, t, 12 + 2 * side : 14 + 2 * side, :] = tile[side, two : two + 2, :]
    for group in groups[6:]:
        start_first(group)
    for group in (*groups[6:], *groups[:6]):
        answer(group)
    for dy in (1, -1):
        copies[0, dy, 0].wait_recv()
    for group in (*groups[6:], *groups[:6]):
        collect(group)

    for s in range(2):
        edge, two = ((23, 22), (16, 16))[s]
        for k in range(2):
            for x in range(NX_L):
                r = (k * 4 + x) * 2
                sp[k, x + 2, two : two + 2, :] = yr[s, r : r + 2, :]
        for axis in range(3):
            for x in range(NX_L):
                r = 16 + axis * 4 + x
                u[axis, x + 1, edge : edge + 1, :] = yr[s, r : r + 1, :]
        for j, i in enumerate(Y_DIRS[s]):
            for x in range(NX_L):
                r = 28 + j * 4 + x
                f1[i, x + 1, edge : edge + 1, :] = yr[s, r : r + 1, :]
    for s in range(2):
        last = 0 if s == 0 else 5
        planes = [(k, layer if s == 0 else 6 + layer) for k in range(2) for layer in range(2)]
        for n, (k, plane) in enumerate(planes):
            sp[k, plane, 0:16, :] = xr[s, n]
        for axis in range(3):
            u[axis, last, 0:16, :] = xr[s, 4 + axis]
        for j, i in enumerate(X_DIRS[s]):
            f1[i, last, 0:16, :] = xr[s, 7 + j]
        for t in range(2):
            edge, two = ((23, 22), (16, 16))[t]
            for n, (k, plane) in enumerate(planes):
                sp[k, plane, two : two + 2, :] = xyr[s, t, 2 * n : 2 * n + 2, :]
            for axis in range(3):
                u[axis, last, edge : edge + 1, :] = xyr[s, t, 8 + axis : 9 + axis, :]
            i = VELOCITIES.index((1 - 2 * s, 1 - 2 * t, 0))
            f1[i, last, edge : edge + 1, :] = xyr[s, t, 11:12, :]

    def merged(own, below, above):
        return jnp.where(part < 2, below, jnp.where(part > 5, above, own))

    def row_tile(n, after, before):
        rest[n, 6:8, :] = before
        rest[n, 0:2, :] = after
        return rest[n]

    def beyond_z(side):
        own, a, b = zr[side], xzr[0, side], xzr[1, side]
        n = side * 3
        third = merged(
            row_tile(n, yzr[1, side], yzr[0, side]),
            roll(row_tile(n + 1, xyzr[0, 1, side], xyzr[0, 0, side]), -4, 1),
            roll(row_tile(n + 2, xyzr[1, 1, side], xyzr[1, 0, side]), 4, 1),
        )
        return jnp.concatenate(
            [merged(own, roll(a, -4, 1), roll(b, 4, 1)), merged(roll(own, -4, 1), roll(a, -8, 1), b), third], axis=0
        )

    def own_z(side):
        n = 6 + side * 3
        r, q = slice(48 + 2 * side, 50 + 2 * side), slice(12 + 2 * side, 14 + 2 * side)
        third = merged(
            row_tile(n, yr[1, r, :], yr[0, r, :]),
            roll(row_tile(n + 1, xyr[0, 1, q, :], xyr[0, 0, q, :]), -4, 1),
            roll(row_tile(n + 2, xyr[1, 1, q, :], xyr[1, 0, q, :]), 4, 1),
        )
        rows = [
            merged(tile[side, h, :], roll(xr[0, 12 + side, h, :], -4, 1), roll(xr[1, 12 + side, h, :], 4, 1))
            for h in (slice(0, 8), slice(8, 16))
        ]
        return jnp.concatenate([*rows, third], axis=0)

    low, high = beyond_z(0), beyond_z(1)
    own_high, own_low = own_z(0), own_z(1)

    for k in range(2):
        for p in range(8):
            a = jnp.abs(sp[k, p])
            above = jnp.where(lane == 127, roll(jnp.abs(high), 127 - (k * 8 + p), 1), roll(a, -1, 1))
            below = jnp.where(lane == 0, roll(jnp.abs(low), -(k * 8 + p), 1), roll(a, 1, 1))
            pz, w = above + below, above - below
            a_up, a_down = roll(a, -1, 0), roll(a, 1, 0)
            gq[k, p] = FACE * a + DIAG * (a_up + a_down + pz)
            v = a_up - a_down
            gv[k, p] = DIAG * v
            gw[k, p] = DIAG * w
            if 1 <= p <= 6:
                gvp[k, p] = FACE * v + DIAG * (roll(pz, -1, 0) - roll(pz, 1, 0))
                gwp[k, p] = FACE * w + DIAG * (roll(w, -1, 0) + roll(w, 1, 0))

    for p in range(1, 7):
        grad = [
            (
                gq[k, p + 1] - gq[k, p - 1],
                gvp[k, p] + gv[k, p + 1] + gv[k, p - 1],
                gwp[k, p] + gw[k, p + 1] + gw[k, p - 1],
            )
            for k in range(2)
        ]
        dirs = X_DIRS[0] if p == 1 else X_DIRS[1] if p == 6 else list(range(19))
        for k in range(2):
            value = sp[k, p]
            vel = [u[axis, p - 1] - (coupling * relax_times[k]) * grad[1 - k][axis] for axis in range(3)]
            for i, item in posts(k, value > 0.0, value, vel, dirs, lambda i: f1[i, p - 1]).items():
                post[k, i, p - 1] = item

    def both(a, va, b, vb):
        return jnp.where(lane < 8, roll(a, -8 * va, 1), roll(b, 8 - 8 * vb, 1))

    value = [both(low, k, high, k) for k in range(2)]
    grad = []
    for k in range(2):
        a = jnp.abs(value[k])
        below = jnp.abs(both(low, 2 + k, own_high, k))
        above = jnp.abs(both(own_low, k, high, 2 + k))
        pz, w = above + below, above - below
        a_up, a_down = roll(a, -1, 0), roll(a, 1, 0)
        q = FACE * a + DIAG * (a_up + a_down + pz)
        v = a_up - a_down
        grad.append(
            (
                roll(q, -1, 1) - roll(q, 1, 1),
                FACE * v + DIAG * (roll(pz, -1, 0) - roll(pz, 1, 0) + roll(v, -1, 1) + roll(v, 1, 1)),
                FACE * w + DIAG * (roll(w, -1, 0) + roll(w, 1, 0) + roll(w, -1, 1) + roll(w, 1, 1)),
            )
        )
    sign = jnp.where(lane < 8, 1.0, -1.0)
    common = [both(low, 4 + axis, high, 4 + axis) for axis in range(3)]
    beyond = [
        posts(
            k,
            value[k] > 0.0,
            jnp.abs(value[k]),
            [sign * (common[axis] - (coupling * relax_times[k]) * grad[1 - k][axis]) for axis in range(3)],
            Z_LOW,
            lambda i: both(low, 7 + Z_LOW.index(i), high, 7 + Z_LOW.index(i)),
        )
        for k in range(2)
    ]

    for k in range(2):
        for i in range(19):
            cx, cy, cz = VELOCITIES[i]
            if cz:
                side = beyond[k][i if cz > 0 else OPPOSITE[i]]
                side = (roll(side, cy, 0) if cy else side)[0:16]
            for x in range(NX_L):
                fluid = flag[x] == 0
                old = f0[i, x] if k == 0 else f1[i, x + 1, 0:16, :]
                if i == 0:
                    moved = post[k, 0, x + 1, 0:16, :]
                else:
                    moved = post[k, i, x + 1 - cx]
                    moved = (roll(moved, cy, 0) if cy else moved)[0:16]
                    if cz > 0:
                        moved = jnp.where(lane16 == 0, roll(side, -(x - cx + 2), 1), roll(moved, 1, 1))
                    elif cz < 0:
                        moved = jnp.where(lane16 == 127, roll(side, 127 - (x - cx + 10), 1), roll(moved, -1, 1))
                    moved = jnp.where(moved < LIMIT, moved, post[k, OPPOSITE[i], x + 1, 0:16, :])
                out[k, i, x] = jnp.where(fluid, moved, old)

    for copy in copies.values():
        copy.wait_send()


def body(populations, solid):
    f32 = jnp.float32
    plane = (ROWS, NZ_L)
    scratch = [
        pltpu.VMEM((19, 4, 16, 128), f32),
        pltpu.VMEM((19, 6, *plane), f32),
        pltpu.VMEM((2, 8, *plane), f32),
        pltpu.VMEM((3, 6, *plane), f32),
        *[pltpu.VMEM((2, 8, *plane), f32)] * 5,
        pltpu.VMEM((2, 19, 6, *plane), f32),
        *[pltpu.VMEM((2, 56, 128), f32)] * 2,
        *[pltpu.VMEM((2, 14, 16, 128), f32)] * 2,
        *[pltpu.VMEM((2, 2, 16, 128), f32)] * 2,
        pltpu.VMEM((2, 16, 128), f32),
        *[pltpu.VMEM((2, 8, 128), f32)] * 2,
        pltpu.VMEM((2, 2, 8, 128), f32),
        *[pltpu.VMEM((2, 2, 2, 128), f32)] * 2,
        pltpu.VMEM((2, 2, 2, 2, 128), f32),
        pltpu.VMEM((12, 8, 128), f32),
        pltpu.SemaphoreType.DMA((2,)),
        pltpu.SemaphoreType.DMA((26,)),
        pltpu.SemaphoreType.DMA((26,)),
    ]
    return pl.pallas_call(
        kernel,
        out_shape=jax.ShapeDtypeStruct(populations.shape, f32),
        in_specs=[pl.BlockSpec(memory_space=pl.ANY), pl.BlockSpec(memory_space=pltpu.VMEM)],
        out_specs=pl.BlockSpec(memory_space=pltpu.VMEM),
        scratch_shapes=scratch,
        compiler_params=pltpu.CompilerParams(
            collective_id=0, has_side_effects=True, vmem_limit_bytes=52 * 1024 * 1024
        ),
    )(populations, solid)


def solution(mesh):
    in_specs = (P(None, None, "gx", "gy", "gz"), P("gx", "gy", "gz"))
    out_specs = P(None, None, "gx", "gy", "gz")
    return jax.shard_map(body, mesh=mesh, in_specs=in_specs, out_specs=out_specs, check_vma=False)
```

```python
import functools

import jax
import jax.numpy as jnp
from jax import lax
from jax.experimental import pallas as pl
from jax.experimental.pallas import tpu as pltpu
from jax.sharding import PartitionSpec as P

VELOCITIES = [
    (0, 0, 0),
    (1, 0, 0),
    (-1, 0, 0),
    (0, 1, 0),
    (0, -1, 0),
    (0, 0, 1),
    (0, 0, -1),
    (1, 1, 0),
    (-1, -1, 0),
    (1, -1, 0),
    (-1, 1, 0),
    (1, 0, 1),
    (-1, 0, -1),
    (1, 0, -1),
    (-1, 0, 1),
    (0, 1, 1),
    (0, -1, -1),
    (0, 1, -1),
    (0, -1, 1),
]
WEIGHTS = [1.0 / 3.0] + [1.0 / 18.0] * 6 + [1.0 / 36.0] * 12
OPPOSITE = [0, 2, 1, 4, 3, 6, 5, 8, 7, 10, 9, 12, 11, 14, 13, 16, 15, 18, 17]
PAIRS = [(1, 2), (3, 4), (5, 6), (7, 8), (9, 10), (11, 12), (13, 14), (15, 16), (17, 18)]
coupling = 0.9
relax_times = (1.0, 0.8)
wall_values = (0.3, 1.5)

NX_L, NY_L, NZ_L = 4, 16, 128
ROWS = 24
X_DIRS = ([i for i in range(19) if VELOCITIES[i][0] == 1], [i for i in range(19) if VELOCITIES[i][0] == -1])
Y_DIRS = ([i for i in range(19) if VELOCITIES[i][1] == 1], [i for i in range(19) if VELOCITIES[i][1] == -1])
Z_LOW = [i for i in range(19) if VELOCITIES[i][2] == 1]
Z_HIGH = [OPPOSITE[i] for i in Z_LOW]
BIG = 1e30
LIMIT = 1e28
FACE, DIAG = 1.0 / 18.0, 1.0 / 36.0
MESH = pl.DeviceIdType.MESH


def roll(a, shift, axis):
    return pltpu.roll(a, shift % a.shape[axis], axis)


def posts(k, fluid, rho, v, dirs, old):
    scale = 1.0 / relax_times[k]
    r = jnp.where(fluid, rho * scale, 0.0)
    b = [1.5 * c for c in v]
    quad = b[0] * b[0] + b[1] * b[1] + b[2] * b[2]
    base = r - (2.0 / 3.0) * r * quad
    base = jnp.where(fluid, base, BIG)
    out = {}

    def keep(i, eq):
        out[i] = eq if k == 0 else eq + (1.0 - scale) * old(i)

    if 0 in dirs:
        keep(0, WEIGHTS[0] * base)
    by_weight = {}
    for pair in PAIRS:
        if not any(i in dirs for i in pair):
            continue
        i = pair[0]
        w = WEIGHTS[i]
        if w not in by_weight:
            by_weight[w] = (w * base, (2.0 * w) * r)
        wb, wr = by_weight[w]
        along = None
        for axis in range(3):
            c = VELOCITIES[i][axis]
            if c:
                along = (b[axis] if c > 0 else -b[axis]) if along is None else (along + b[axis] if c > 0 else along - b[axis])
        t = wr * along
        s = wb + along * t
        if i in dirs:
            keep(i, s + t)
        if pair[1] in dirs:
            keep(pair[1], s - t)
    return out


def index_of(c):
    return 0 if c > 0 else 1


def ahead(ix, iz, nx, nz, dx, dz):
    if dz:
        rank = (lambda g: jnp.where(g < 2, g, 5 - g)) if nz == 4 else (lambda g: g)
        return rank(iz) > rank(lax.rem(iz + dz + nz, nz))
    if dx:
        return lax.rem(ix, 4) > lax.rem(lax.rem(ix + dx + nx, nx), 4)
    return None


def both_signal(ix, iz, nx, nz, dx, dz):
    if dx * dz >= 0:
        return jnp.bool_(False)
    return (ix == 0) & (iz == nz - 2) if dz > 0 else (ix == nx - 1) & (iz == nz - 1)


def kernel(
    pop, solid, out, flag, f0, f1, sp, u, gq, gvp, gv, gwp, gw, post,
    ys, yr, xs, xr, xys, xyr, tile, zs, zr, xzr, ps, yzr, xyzr, rest, sem_in, send, recv,
):
    ix, iy, iz = lax.axis_index("gx"), lax.axis_index("gy"), lax.axis_index("gz")
    nx, ny, nz = lax.axis_size("gx"), lax.axis_size("gy"), lax.axis_size("gz")
    around = (0, 1, -1)
    groups = [(dx, dz) for dz in (1, -1) for dx in around] + [(1, 0), (-1, 0)]
    leads = {g: ahead(ix, iz, nx, nz, *g) for g in groups}
    mutual = {g: both_signal(ix, iz, nx, nz, *g) for g in groups}
    sends_first = {g: leads[g] | mutual[g] for g in groups}

    def target(dx, dy, dz):
        place = {}
        if dx:
            place["gx"] = lax.rem(ix + dx + nx, nx)
        if dy:
            place["gy"] = lax.rem(iy + dy + ny, ny)
        if dz:
            place["gz"] = lax.rem(iz + dz + nz, nz)
        return place

    loads = [
        pltpu.make_async_copy(solid, flag, sem_in.at[2]),
        pltpu.make_async_copy(pop.at[0], f0, sem_in.at[0]),
        pltpu.make_async_copy(pop.at[1], f1.at[:, 1:5, 0:16, :], sem_in.at[1]),
    ]
    for copy in loads:
        copy.start()
    barrier = pltpu.get_barrier_semaphore()
    count = 2
    for dx, dz in groups:
        first = sends_first[dx, dz]
        count = count + 3 * first.astype(jnp.int32)

        @pl.when(jnp.logical_not(leads[dx, dz]) | mutual[dx, dz])
        def _(dx=dx, dz=dz):
            for dy in around:
                pl.semaphore_signal(barrier, inc=1, device_id=target(dx, dy, dz), device_id_type=MESH)

    for dy in (1, -1):
        pl.semaphore_signal(barrier, inc=1, device_id=target(0, dy, 0), device_id_type=MESH)

    ways = [(dx, dy, dz) for dz in around for dx in around for dy in around if dx or dy or dz]
    copies = {}
    for n, (dx, dy, dz) in enumerate(ways):
        x, y, z = index_of(dx), index_of(dy), index_of(dz)
        if dz:
            src = ps.at[z, y] if dy else zs.at[z]
            if dx:
                dst = xyzr.at[x, y, z] if dy else xzr.at[x, z]
            else:
                dst = yzr.at[y, z] if dy else zr.at[z]
        elif dx:
            src, dst = (xys.at[x, y], xyr.at[x, y]) if dy else (xs.at[x], xr.at[x])
        else:
            src, dst = ys.at[y], yr.at[y]
        copies[dx, dy, dz] = pltpu.make_async_remote_copy(
            src_ref=src, dst_ref=dst, send_sem=send.at[n], recv_sem=recv.at[n],
            device_id=target(dx, dy, dz), device_id_type=MESH,
        )

    for copy in loads:
        copy.wait()

    for x in range(NX_L):
        fluid = flag[x] == 0
        rho, momentum = [], []
        for k in range(2):
            f = (lambda i: f0[i, x]) if k == 0 else (lambda i: f1[i, x + 1, 0:16, :])
            total = f(0)
            mom = [None, None, None]
            for i, j in PAIRS:
                a, b = f(i), f(j)
                total = total + (a + b)
                d = a - b
                for axis in range(3):
                    c = VELOCITIES[i][axis]
                    if c:
                        mom[axis] = d * float(c) if mom[axis] is None else (mom[axis] + d if c > 0 else mom[axis] - d)
            rho.append(total)
            momentum.append(mom)
            sp[k, x + 2, 0:16, :] = jnp.where(fluid, total, -wall_values[k])
        inv = 1.0 / (rho[0] * (1.0 / relax_times[0]) + rho[1] * (1.0 / relax_times[1]))
        for axis in range(3):
            u[axis, x + 1, 0:16, :] = (
                momentum[0][axis] * (1.0 / relax_times[0]) + momentum[1][axis] * (1.0 / relax_times[1])
            ) * inv

    lane = lax.broadcasted_iota(jnp.int32, (ROWS, NZ_L), 1)
    lane16 = lax.broadcasted_iota(jnp.int32, (NY_L, NZ_L), 1)
    part = lax.broadcasted_iota(jnp.int32, (8, NZ_L), 1) % 8

    for s in range(2):
        near, far = ((127, 126), (0, 1))[s]
        dirs = (Z_LOW, Z_HIGH)[s]
        packed = jnp.zeros((NY_L, NZ_L), jnp.float32)
        for v in range(12):
            for x in range(NX_L):
                if v < 4:
                    value, column = sp[v % 2, x + 2, 0:16, :], near if v < 2 else far
                elif v < 7:
                    value, column = u[v - 4, x + 1, 0:16, :], near
                else:
                    value, column = f1[dirs[v - 7], x + 1, 0:16, :], near
                spot = v * 8 + x + 2
                packed = jnp.where(lane16 == spot, roll(value, spot - column, 1), packed)
        tile[s] = packed
        zs[s] = jnp.where((part >= 2) & (part <= 5), packed[0:8], roll(packed[8:16], 4, 1))
        ps[s, 0] = packed[14:16]
        ps[s, 1] = packed[0:2]

    def start_first(group):
        @pl.when(sends_first[group])
        def _():
            for dy in around:
                copies[group[0], dy, group[1]].start()

    def answer(group):
        @pl.when(jnp.logical_not(sends_first[group]))
        def _():
            for dy in around:
                copies[-group[0], -dy, -group[1]].wait_recv()
                copies[group[0], dy, group[1]].start()

    def collect(group):
        @pl.when(sends_first[group])
        def _():
            for dy in around:
                copies[-group[0], -dy, -group[1]].wait_recv()

    pl.semaphore_wait(barrier, count)
    for group in groups[:6]:
        start_first(group)

    for s in range(2):
        edge, two = ((15, 14), (0, 0))[s]
        for k in range(2):
            for x in range(NX_L):
                r = (k * 4 + x) * 2
                ys[s, r : r + 2, :] = sp[k, x + 2, two : two + 2, :]
        for axis in range(3):
            for x in range(NX_L):
                r = 16 + axis * 4 + x
                ys[s, r : r + 1, :] = u[axis, x + 1, edge : edge + 1, :]
        for j, i in enumerate(Y_DIRS[s]):
            for x in range(NX_L):
                r = 28 + j * 4 + x
                ys[s, r : r + 1, :] = f1[i, x + 1, edge : edge + 1, :]
        for side in range(2):
            ys[s, 48 + 2 * side : 50 + 2 * side, :] = tile[side, two : two + 2, :]
    for dy in (1, -1):
        copies[0, dy, 0].start()
    for s in range(2):
        last = 4 if s == 0 else 1
        planes = [(k, 2 + (2 + layer if s == 0 else layer)) for k in range(2) for layer in range(2)]
        for n, (k, plane) in enumerate(planes):
            xs[s, n] = sp[k, plane, 0:16, :]
        for axis in range(3):
            xs[s, 4 + axis] = u[axis, last, 0:16, :]
        for j, i in enumerate(X_DIRS[s]):
            xs[s, 7 + j] = f1[i, last, 0:16, :]
        for side in range(2):
            xs[s, 12 + side] = tile[side]
        for t in range(2):
            edge, two = ((15, 14), (0, 0))[t]
            for n, (k, plane) in enumerate(planes):
                xys[s, t, 2 * n : 2 * n + 2, :] = sp[k, plane, two : two + 2, :]
            for axis in range(3):
                xys[s, t, 8 + axis : 9 + axis, :] = u[axis, last, edge : edge + 1, :]
            i = VELOCITIES.index((1 - 2 * s, 1 - 2 * t, 0))
            xys[s, t, 11:12, :] = f1[i, last, edge : edge + 1, :]
            for side in range(2):
                xys[s, t, 12 + 2 * side : 14 + 2 * side, :] = tile[side, two : two + 2, :]
    for group in groups[6:]:
        start_first(group)
    for group in (*groups[6:], *groups[:6]):
        answer(group)
    for dy in (1, -1):
        copies[0, dy, 0].wait_recv()
    for group in (*groups[6:], *groups[:6]):
        collect(group)

    for s in range(2):
        edge, two = ((23, 22), (16, 16))[s]
        for k in range(2):
            for x in range(NX_L):
                r = (k * 4 + x) * 2
                sp[k, x + 2, two : two + 2, :] = yr[s, r : r + 2, :]
        for axis in range(3):
            for x in range(NX_L):
                r = 16 + axis * 4 + x
                u[axis, x + 1, edge : edge + 1, :] = yr[s, r : r + 1, :]
        for j, i in enumerate(Y_DIRS[s]):
            for x in range(NX_L):
                r = 28 + j * 4 + x
                f1[i, x + 1, edge : edge + 1, :] = yr[s, r : r + 1, :]
    for s in range(2):
        last = 0 if s == 0 else 5
        planes = [(k, layer if s == 0 else 6 + layer) for k in range(2) for layer in range(2)]
        for n, (k, plane) in enumerate(planes):
            sp[k, plane, 0:16, :] = xr[s, n]
        for axis in range(3):
            u[axis, last, 0:16, :] = xr[s, 4 + axis]
        for j, i in enumerate(X_DIRS[s]):
            f1[i, last, 0:16, :] = xr[s, 7 + j]
        for t in range(2):
            edge, two = ((23, 22), (16, 16))[t]
            for n, (k, plane) in enumerate(planes):
                sp[k, plane, two : two + 2, :] = xyr[s, t, 2 * n : 2 * n + 2, :]
            for axis in range(3):
                u[axis, last, edge : edge + 1, :] = xyr[s, t, 8 + axis : 9 + axis, :]
            i = VELOCITIES.index((1 - 2 * s, 1 - 2 * t, 0))
            f1[i, last, edge : edge + 1, :] = xyr[s, t, 11:12, :]

    def merged(own, below, above):
        return jnp.where(part < 2, below, jnp.where(part > 5, above, own))

    def row_tile(n, after, before):
        rest[n, 6:8, :] = before
        rest[n, 0:2, :] = after
        return rest[n]

    def beyond_z(side):
        own, a, b = zr[side], xzr[0, side], xzr[1, side]
        n = side * 3
        third = merged(
            row_tile(n, yzr[1, side], yzr[0, side]),
            roll(row_tile(n + 1, xyzr[0, 1, side], xyzr[0, 0, side]), -4, 1),
            roll(row_tile(n + 2, xyzr[1, 1, side], xyzr[1, 0, side]), 4, 1),
        )
        return jnp.concatenate(
            [merged(own, roll(a, -4, 1), roll(b, 4, 1)), merged(roll(own, -4, 1), roll(a, -8, 1), b), third], axis=0
        )

    def own_z(side):
        n = 6 + side * 3
        r, q = slice(48 + 2 * side, 50 + 2 * side), slice(12 + 2 * side, 14 + 2 * side)
        third = merged(
            row_tile(n, yr[1, r, :], yr[0, r, :]),
            roll(row_tile(n + 1, xyr[0, 1, q, :], xyr[0, 0, q, :]), -4, 1),
            roll(row_tile(n + 2, xyr[1, 1, q, :], xyr[1, 0, q, :]), 4, 1),
        )
        rows = [
            merged(tile[side, h, :], roll(xr[0, 12 + side, h, :], -4, 1), roll(xr[1, 12 + side, h, :], 4, 1))
            for h in (slice(0, 8), slice(8, 16))
        ]
        return jnp.concatenate([*rows, third], axis=0)

    low, high = beyond_z(0), beyond_z(1)
    own_high, own_low = own_z(0), own_z(1)

    for k in range(2):
        for p in range(8):
            a = jnp.abs(sp[k, p])
            above = jnp.where(lane == 127, roll(jnp.abs(high), 127 - (k * 8 + p), 1), roll(a, -1, 1))
            below = jnp.where(lane == 0, roll(jnp.abs(low), -(k * 8 + p), 1), roll(a, 1, 1))
            pz, w = above + below, above - below
            a_up, a_down = roll(a, -1, 0), roll(a, 1, 0)
            gq[k, p] = FACE * a + DIAG * (a_up + a_down + pz)
            v = a_up - a_down
            gv[k, p] = DIAG * v
            gw[k, p] = DIAG * w
            if 1 <= p <= 6:
                gvp[k, p] = FACE * v + DIAG * (roll(pz, -1, 0) - roll(pz, 1, 0))
                gwp[k, p] = FACE * w + DIAG * (roll(w, -1, 0) + roll(w, 1, 0))

    for p in range(1, 7):
        grad = [
            (
                gq[k, p + 1] - gq[k, p - 1],
                gvp[k, p] + gv[k, p + 1] + gv[k, p - 1],
                gwp[k, p] + gw[k, p + 1] + gw[k, p - 1],
            )
            for k in range(2)
        ]
        dirs = X_DIRS[0] if p == 1 else X_DIRS[1] if p == 6 else list(range(19))
        for k in range(2):
            value = sp[k, p]
            vel = [u[axis, p - 1] - (coupling * relax_times[k]) * grad[1 - k][axis] for axis in range(3)]
            for i, item in posts(k, value > 0.0, value, vel, dirs, lambda i: f1[i, p - 1]).items():
                post[k, i, p - 1] = item

    def both(a, va, b, vb):
        return jnp.where(lane < 8, roll(a, -8 * va, 1), roll(b, 8 - 8 * vb, 1))

    value = [both(low, k, high, k) for k in range(2)]
    grad = []
    for k in range(2):
        a = jnp.abs(value[k])
        below = jnp.abs(both(low, 2 + k, own_high, k))
        above = jnp.abs(both(own_low, k, high, 2 + k))
        pz, w = above + below, above - below
        a_up, a_down = roll(a, -1, 0), roll(a, 1, 0)
        q = FACE * a + DIAG * (a_up + a_down + pz)
        v = a_up - a_down
        grad.append(
            (
                roll(q, -1, 1) - roll(q, 1, 1),
                FACE * v + DIAG * (roll(pz, -1, 0) - roll(pz, 1, 0) + roll(v, -1, 1) + roll(v, 1, 1)),
                FACE * w + DIAG * (roll(w, -1, 0) + roll(w, 1, 0) + roll(w, -1, 1) + roll(w, 1, 1)),
            )
        )
    sign = jnp.where(lane < 8, 1.0, -1.0)
    common = [both(low, 4 + axis, high, 4 + axis) for axis in range(3)]
    beyond = [
        posts(
            k,
            value[k] > 0.0,
            jnp.abs(value[k]),
            [sign * (common[axis] - (coupling * relax_times[k]) * grad[1 - k][axis]) for axis in range(3)],
            Z_LOW,
            lambda i: both(low, 7 + Z_LOW.index(i), high, 7 + Z_LOW.index(i)),
        )
        for k in range(2)
    ]

    for k in range(2):
        for i in range(19):
            cx, cy, cz = VELOCITIES[i]
            if cz:
                side = beyond[k][i if cz > 0 else OPPOSITE[i]]
                side = (roll(side, cy, 0) if cy else side)[0:16]
            for x in range(NX_L):
                fluid = flag[x] == 0
                old = f0[i, x] if k == 0 else f1[i, x + 1, 0:16, :]
                if i == 0:
                    moved = post[k, 0, x + 1, 0:16, :]
                else:
                    moved = post[k, i, x + 1 - cx]
                    moved = (roll(moved, cy, 0) if cy else moved)[0:16]
                    if cz > 0:
                        moved = jnp.where(lane16 == 0, roll(side, -(x - cx + 2), 1), roll(moved, 1, 1))
                    elif cz < 0:
                        moved = jnp.where(lane16 == 127, roll(side, 127 - (x - cx + 10), 1), roll(moved, -1, 1))
                    moved = jnp.where(moved < LIMIT, moved, post[k, OPPOSITE[i], x + 1, 0:16, :])
                out[k, i, x] = jnp.where(fluid, moved, old)

    for copy in copies.values():
        copy.wait_send()


def body(populations, solid):
    f32 = jnp.float32
    plane = (ROWS, NZ_L)
    scratch = [
        pltpu.VMEM((4, 16, 128), jnp.int32),
        pltpu.VMEM((19, 4, 16, 128), f32),
        pltpu.VMEM((19, 6, *plane), f32),
        pltpu.VMEM((2, 8, *plane), f32),
        pltpu.VMEM((3, 6, *plane), f32),
        *[pltpu.VMEM((2, 8, *plane), f32)] * 5,
        pltpu.VMEM((2, 19, 6, *plane), f32),
        *[pltpu.VMEM((2, 56, 128), f32)] * 2,
        *[pltpu.VMEM((2, 14, 16, 128), f32)] * 2,
        *[pltpu.VMEM((2, 2, 16, 128), f32)] * 2,
        pltpu.VMEM((2, 16, 128), f32),
        *[pltpu.VMEM((2, 8, 128), f32)] * 2,
        pltpu.VMEM((2, 2, 8, 128), f32),
        *[pltpu.VMEM((2, 2, 2, 128), f32)] * 2,
        pltpu.VMEM((2, 2, 2, 2, 128), f32),
        pltpu.VMEM((12, 8, 128), f32),
        pltpu.SemaphoreType.DMA((3,)),
        pltpu.SemaphoreType.DMA((26,)),
        pltpu.SemaphoreType.DMA((26,)),
    ]
    return pl.pallas_call(
        kernel,
        out_shape=jax.ShapeDtypeStruct(populations.shape, f32),
        in_specs=[pl.BlockSpec(memory_space=pltpu.HBM)] * 2,
        out_specs=pl.BlockSpec(memory_space=pltpu.VMEM),
        scratch_shapes=scratch,
        compiler_params=pltpu.CompilerParams(
            collective_id=0, has_side_effects=True, vmem_limit_bytes=40 * 1024 * 1024
        ),
    )(*[pltpu.with_memory_space_constraint(a, pltpu.HBM) for a in (populations, solid)])


def solution(mesh):
    in_specs = (P(None, None, "gx", "gy", "gz"), P("gx", "gy", "gz"))
    out_specs = P(None, None, "gx", "gy", "gz")
    return jax.shard_map(body, mesh=mesh, in_specs=in_specs, out_specs=out_specs, check_vma=False)
```

```python
import functools

import jax
import jax.numpy as jnp
from jax import lax
from jax.experimental import pallas as pl
from jax.experimental.pallas import tpu as pltpu
from jax.sharding import PartitionSpec as P

VELOCITIES = [
    (0, 0, 0),
    (1, 0, 0),
    (-1, 0, 0),
    (0, 1, 0),
    (0, -1, 0),
    (0, 0, 1),
    (0, 0, -1),
    (1, 1, 0),
    (-1, -1, 0),
    (1, -1, 0),
    (-1, 1, 0),
    (1, 0, 1),
    (-1, 0, -1),
    (1, 0, -1),
    (-1, 0, 1),
    (0, 1, 1),
    (0, -1, -1),
    (0, 1, -1),
    (0, -1, 1),
]
WEIGHTS = [1.0 / 3.0] + [1.0 / 18.0] * 6 + [1.0 / 36.0] * 12
OPPOSITE = [0, 2, 1, 4, 3, 6, 5, 8, 7, 10, 9, 12, 11, 14, 13, 16, 15, 18, 17]
PAIRS = [(1, 2), (3, 4), (5, 6), (7, 8), (9, 10), (11, 12), (13, 14), (15, 16), (17, 18)]
coupling = 0.9
relax_times = (1.0, 0.8)
wall_values = (0.3, 1.5)

NX_L, NY_L, NZ_L = 4, 16, 128
ROWS = 24
X_DIRS = ([i for i in range(19) if VELOCITIES[i][0] == 1], [i for i in range(19) if VELOCITIES[i][0] == -1])
Y_DIRS = ([i for i in range(19) if VELOCITIES[i][1] == 1], [i for i in range(19) if VELOCITIES[i][1] == -1])
Z_LOW = [i for i in range(19) if VELOCITIES[i][2] == 1]
Z_HIGH = [OPPOSITE[i] for i in Z_LOW]
BIG = 1e30
LIMIT = 1e28
FACE, DIAG = 1.0 / 18.0, 1.0 / 36.0
MESH = pl.DeviceIdType.MESH


def roll(a, shift, axis):
    return pltpu.roll(a, shift % a.shape[axis], axis)


def posts(k, fluid, rho, v, dirs, old):
    scale = 1.0 / relax_times[k]
    r = jnp.where(fluid, rho * scale, 0.0)
    b = [1.5 * c for c in v]
    quad = b[0] * b[0] + b[1] * b[1] + b[2] * b[2]
    base = r - (2.0 / 3.0) * r * quad
    base = jnp.where(fluid, base, BIG)
    out = {}

    def keep(i, eq):
        out[i] = eq if k == 0 else eq + (1.0 - scale) * old(i)

    if 0 in dirs:
        keep(0, WEIGHTS[0] * base)
    by_weight = {}
    for pair in PAIRS:
        if not any(i in dirs for i in pair):
            continue
        i = pair[0]
        w = WEIGHTS[i]
        if w not in by_weight:
            by_weight[w] = (w * base, (2.0 * w) * r)
        wb, wr = by_weight[w]
        along = None
        for axis in range(3):
            c = VELOCITIES[i][axis]
            if c:
                along = (b[axis] if c > 0 else -b[axis]) if along is None else (along + b[axis] if c > 0 else along - b[axis])
        t = wr * along
        s = wb + along * t
        if i in dirs:
            keep(i, s + t)
        if pair[1] in dirs:
            keep(pair[1], s - t)
    return out


def index_of(c):
    return 0 if c > 0 else 1


def ahead(ix, iz, nx, nz, dx, dz):
    if dz:
        rank = (lambda g: jnp.where(g < 2, g, 5 - g)) if nz == 4 else (lambda g: -g)
        return rank(iz) > rank(lax.rem(iz + dz + nz, nz))
    if dx:
        return lax.rem(ix, 4) > lax.rem(lax.rem(ix + dx + nx, nx), 4)
    return None


def vouched(ix, iz, nx, nz, dx, dz):
    if dx * dz >= 0:
        return jnp.bool_(False)
    return (ix == 0) & (iz == nz - 2) if dz > 0 else (ix == nx - 1) & (iz == nz - 1)


def kernel(
    pop, solid, out, flag, f0, f1, sp, u, gq, gvp, gv, gwp, gw, post,
    ys, yr, xs, xr, xys, xyr, tile, zs, zr, xzr, ps, yzr, xyzr, rest, sem_in, send, recv, go, vouch,
):
    ix, iy, iz = lax.axis_index("gx"), lax.axis_index("gy"), lax.axis_index("gz")
    nx, ny, nz = lax.axis_size("gx"), lax.axis_size("gy"), lax.axis_size("gz")
    around = (0, 1, -1)
    groups = [(dx, dz) for dz in (1, -1) for dx in around] + [(1, 0), (-1, 0)]
    leads = {g: ahead(ix, iz, nx, nz, *g) for g in groups}
    told = {g: vouched(ix, iz, nx, nz, *g) for g in groups}
    sends_first = {g: leads[g] & jnp.logical_not(told[g]) for g in groups}
    answers = {g: jnp.logical_not(leads[g] | told[g]) for g in groups}

    def target(dx, dy, dz):
        place = {}
        if dx:
            place["gx"] = lax.rem(ix + dx + nx, nx)
        if dy:
            place["gy"] = lax.rem(iy + dy + ny, ny)
        if dz:
            place["gz"] = lax.rem(iz + dz + nz, nz)
        return place

    mask_load = pltpu.make_async_copy(solid, flag, sem_in.at[8])
    loads = [
        (
            pltpu.make_async_copy(pop.at[0, :, x], f0.at[:, x], sem_in.at[2 * x]),
            pltpu.make_async_copy(pop.at[1, :, x], f1.at[:, x + 1, 0:16, :], sem_in.at[2 * x + 1]),
        )
        for x in range(NX_L)
    ]
    mask_load.start()
    for pair in loads:
        for copy in pair:
            copy.start()
    barrier = pltpu.get_barrier_semaphore()
    count = 2
    for dx, dz in groups:
        first = sends_first[dx, dz]
        count = count + 3 * first.astype(jnp.int32)

        @pl.when(answers[dx, dz])
        def _(dx=dx, dz=dz):
            for dy in around:
                pl.semaphore_signal(barrier, inc=1, device_id=target(dx, dy, dz), device_id_type=MESH)

    for dy in (1, -1):
        pl.semaphore_signal(barrier, inc=1, device_id=target(0, dy, 0), device_id_type=MESH)

    ways = [(dx, dy, dz) for dz in around for dx in around for dy in around if dx or dy or dz]
    copies = {}
    for n, (dx, dy, dz) in enumerate(ways):
        x, y, z = index_of(dx), index_of(dy), index_of(dz)
        if dz:
            src = ps.at[z, y] if dy else zs.at[z]
            if dx:
                dst = xyzr.at[x, y, z] if dy else xzr.at[x, z]
            else:
                dst = yzr.at[y, z] if dy else zr.at[z]
        elif dx:
            src, dst = (xys.at[x, y], xyr.at[x, y]) if dy else (xs.at[x], xr.at[x])
        else:
            src, dst = ys.at[y], yr.at[y]
        copies[dx, dy, dz] = pltpu.make_async_remote_copy(
            src_ref=src, dst_ref=dst, send_sem=send.at[n], recv_sem=recv.at[n],
            device_id=target(dx, dy, dz), device_id_type=MESH,
        )

    lane = lax.broadcasted_iota(jnp.int32, (ROWS, NZ_L), 1)
    lane16 = lax.broadcasted_iota(jnp.int32, (NY_L, NZ_L), 1)
    part = lax.broadcasted_iota(jnp.int32, (8, NZ_L), 1) % 8

    mask_load.wait()
    packed = [jnp.zeros((NY_L, NZ_L), jnp.float32) for s in range(2)]
    for x in range(NX_L):
        for copy in loads[x]:
            copy.wait()
        fluid = flag[x] == 0
        rho, momentum = [], []
        for k in range(2):
            f = (lambda i: f0[i, x]) if k == 0 else (lambda i: f1[i, x + 1, 0:16, :])
            total = f(0)
            mom = [None, None, None]
            for i, j in PAIRS:
                a, b = f(i), f(j)
                total = total + (a + b)
                d = a - b
                for axis in range(3):
                    c = VELOCITIES[i][axis]
                    if c:
                        mom[axis] = d * float(c) if mom[axis] is None else (mom[axis] + d if c > 0 else mom[axis] - d)
            rho.append(total)
            momentum.append(mom)
            sp[k, x + 2, 0:16, :] = jnp.where(fluid, total, -wall_values[k])
        inv = 1.0 / (rho[0] * (1.0 / relax_times[0]) + rho[1] * (1.0 / relax_times[1]))
        for axis in range(3):
            u[axis, x + 1, 0:16, :] = (
                momentum[0][axis] * (1.0 / relax_times[0]) + momentum[1][axis] * (1.0 / relax_times[1])
            ) * inv

        for s in range(2):
            near, far = ((127, 126), (0, 1))[s]
            dirs = (Z_LOW, Z_HIGH)[s]
            for v in range(12):
                if v < 4:
                    value, column = sp[v % 2, x + 2, 0:16, :], near if v < 2 else far
                elif v < 7:
                    value, column = u[v - 4, x + 1, 0:16, :], near
                else:
                    value, column = f1[dirs[v - 7], x + 1, 0:16, :], near
                spot = v * 8 + x + 2
                packed[s] = jnp.where(lane16 == spot, roll(value, spot - column, 1), packed[s])
    for s in range(2):
        tile[s] = packed[s]
        zs[s] = jnp.where((part >= 2) & (part <= 5), packed[s][0:8], roll(packed[s][8:16], 4, 1))
        ps[s, 0] = packed[s][14:16]
        ps[s, 1] = packed[s][0:2]

    def start_first(group):
        @pl.when(sends_first[group])
        def _():
            for dy in around:
                copies[group[0], dy, group[1]].start()

    def admit(group):
        @pl.when(sends_first[group])
        def _():
            for dy in around:
                way = (group[0], dy, group[1])
                pl.semaphore_signal(go.at[ways.index(way)], inc=1, device_id=target(*way), device_id_type=MESH)

    def answer(group):
        @pl.when(answers[group])
        def _():
            for dy in around:
                pl.semaphore_wait(go.at[ways.index((-group[0], -dy, -group[1]))], 1)
                copies[group[0], dy, group[1]].start()

    def collect(group):
        for dy in around:
            copies[-group[0], -dy, -group[1]].wait_recv()

    pl.semaphore_wait(barrier, count)
    for group in groups:
        admit(group)

    @pl.when((ix == nx - 1) & (iz == nz - 2))
    def _():
        pl.semaphore_signal(vouch, inc=1, device_id=target(1, 0, 0), device_id_type=MESH)
        pl.semaphore_signal(vouch, inc=1, device_id=target(0, 0, 1), device_id_type=MESH)
    for group in groups[:6]:
        start_first(group)

    for s in range(2):
        edge, two = ((15, 14), (0, 0))[s]
        for k in range(2):
            for x in range(NX_L):
                r = (k * 4 + x) * 2
                ys[s, r : r + 2, :] = sp[k, x + 2, two : two + 2, :]
        for axis in range(3):
            for x in range(NX_L):
                r = 16 + axis * 4 + x
                ys[s, r : r + 1, :] = u[axis, x + 1, edge : edge + 1, :]
        for j, i in enumerate(Y_DIRS[s]):
            for x in range(NX_L):
                r = 28 + j * 4 + x
                ys[s, r : r + 1, :] = f1[i, x + 1, edge : edge + 1, :]
        for side in range(2):
            ys[s, 48 + 2 * side : 50 + 2 * side, :] = tile[side, two : two + 2, :]
    for dy in (1, -1):
        copies[0, dy, 0].start()
    for s in range(2):
        last = 4 if s == 0 else 1
        planes = [(k, 2 + (2 + layer if s == 0 else layer)) for k in range(2) for layer in range(2)]
        for n, (k, plane) in enumerate(planes):
            xs[s, n] = sp[k, plane, 0:16, :]
        for axis in range(3):
            xs[s, 4 + axis] = u[axis, last, 0:16, :]
        for j, i in enumerate(X_DIRS[s]):
            xs[s, 7 + j] = f1[i, last, 0:16, :]
        for side in range(2):
            xs[s, 12 + side] = tile[side]
        for t in range(2):
            edge, two = ((15, 14), (0, 0))[t]
            for n, (k, plane) in enumerate(planes):
                xys[s, t, 2 * n : 2 * n + 2, :] = sp[k, plane, two : two + 2, :]
            for axis in range(3):
                xys[s, t, 8 + axis : 9 + axis, :] = u[axis, last, edge : edge + 1, :]
            i = VELOCITIES.index((1 - 2 * s, 1 - 2 * t, 0))
            xys[s, t, 11:12, :] = f1[i, last, edge : edge + 1, :]
            for side in range(2):
                xys[s, t, 12 + 2 * side : 14 + 2 * side, :] = tile[side, two : two + 2, :]
    for group in groups[6:]:
        start_first(group)
    def take_plane():
        for dy in (1, -1):
            copies[0, dy, 0].wait_recv()
        for group in groups[6:]:
            collect(group)
        for s in range(2):
            edge, two = ((23, 22), (16, 16))[s]
            for k in range(2):
                for x in range(NX_L):
                    r = (k * 4 + x) * 2
                    sp[k, x + 2, two : two + 2, :] = yr[s, r : r + 2, :]
            for axis in range(3):
                for x in range(NX_L):
                    r = 16 + axis * 4 + x
                    u[axis, x + 1, edge : edge + 1, :] = yr[s, r : r + 1, :]
            for j, i in enumerate(Y_DIRS[s]):
                for x in range(NX_L):
                    r = 28 + j * 4 + x
                    f1[i, x + 1, edge : edge + 1, :] = yr[s, r : r + 1, :]
        for s in range(2):
            last = 0 if s == 0 else 5
            planes = [(k, layer if s == 0 else 6 + layer) for k in range(2) for layer in range(2)]
            for n, (k, plane) in enumerate(planes):
                sp[k, plane, 0:16, :] = xr[s, n]
            for axis in range(3):
                u[axis, last, 0:16, :] = xr[s, 4 + axis]
            for j, i in enumerate(X_DIRS[s]):
                f1[i, last, 0:16, :] = xr[s, 7 + j]
            for t in range(2):
                edge, two = ((23, 22), (16, 16))[t]
                for n, (k, plane) in enumerate(planes):
                    sp[k, plane, two : two + 2, :] = xyr[s, t, 2 * n : 2 * n + 2, :]
                for axis in range(3):
                    u[axis, last, edge : edge + 1, :] = xyr[s, t, 8 + axis : 9 + axis, :]
                i = VELOCITIES.index((1 - 2 * s, 1 - 2 * t, 0))
                f1[i, last, edge : edge + 1, :] = xyr[s, t, 11:12, :]

    for group in groups[6:]:
        answer(group)
    for group in groups[:6]:
        answer(group)
    for group in ((1, -1), (-1, 1)):

        @pl.when(told[group])
        def _(group=group):
            pl.semaphore_wait(vouch, 1)
            for dy in around:
                copies[group[0], dy, group[1]].start()

    take_plane()
    for group in groups[:6]:
        collect(group)

    def merged(own, below, above):
        return jnp.where(part < 2, below, jnp.where(part > 5, above, own))

    def row_tile(n, after, before):
        rest[n, 6:8, :] = before
        rest[n, 0:2, :] = after
        return rest[n]

    def beyond_z(side):
        own, a, b = zr[side], xzr[0, side], xzr[1, side]
        n = side * 3
        third = merged(
            row_tile(n, yzr[1, side], yzr[0, side]),
            roll(row_tile(n + 1, xyzr[0, 1, side], xyzr[0, 0, side]), -4, 1),
            roll(row_tile(n + 2, xyzr[1, 1, side], xyzr[1, 0, side]), 4, 1),
        )
        return jnp.concatenate(
            [merged(own, roll(a, -4, 1), roll(b, 4, 1)), merged(roll(own, -4, 1), roll(a, -8, 1), b), third], axis=0
        )

    def own_z(side):
        n = 6 + side * 3
        r, q = slice(48 + 2 * side, 50 + 2 * side), slice(12 + 2 * side, 14 + 2 * side)
        third = merged(
            row_tile(n, yr[1, r, :], yr[0, r, :]),
            roll(row_tile(n + 1, xyr[0, 1, q, :], xyr[0, 0, q, :]), -4, 1),
            roll(row_tile(n + 2, xyr[1, 1, q, :], xyr[1, 0, q, :]), 4, 1),
        )
        rows = [
            merged(tile[side, h, :], roll(xr[0, 12 + side, h, :], -4, 1), roll(xr[1, 12 + side, h, :], 4, 1))
            for h in (slice(0, 8), slice(8, 16))
        ]
        return jnp.concatenate([*rows, third], axis=0)

    low, high = beyond_z(0), beyond_z(1)
    own_high, own_low = own_z(0), own_z(1)

    for k in range(2):
        for p in range(8):
            a = jnp.abs(sp[k, p])
            above = jnp.where(lane == 127, roll(jnp.abs(high), 127 - (k * 8 + p), 1), roll(a, -1, 1))
            below = jnp.where(lane == 0, roll(jnp.abs(low), -(k * 8 + p), 1), roll(a, 1, 1))
            pz, w = above + below, above - below
            a_up, a_down = roll(a, -1, 0), roll(a, 1, 0)
            gq[k, p] = FACE * a + DIAG * (a_up + a_down + pz)
            v = a_up - a_down
            gv[k, p] = DIAG * v
            gw[k, p] = DIAG * w
            if 1 <= p <= 6:
                gvp[k, p] = FACE * v + DIAG * (roll(pz, -1, 0) - roll(pz, 1, 0))
                gwp[k, p] = FACE * w + DIAG * (roll(w, -1, 0) + roll(w, 1, 0))

    for p in range(1, 7):
        grad = [
            (
                gq[k, p + 1] - gq[k, p - 1],
                gvp[k, p] + gv[k, p + 1] + gv[k, p - 1],
                gwp[k, p] + gw[k, p + 1] + gw[k, p - 1],
            )
            for k in range(2)
        ]
        dirs = X_DIRS[0] if p == 1 else X_DIRS[1] if p == 6 else list(range(19))
        for k in range(2):
            value = sp[k, p]
            vel = [u[axis, p - 1] - (coupling * relax_times[k]) * grad[1 - k][axis] for axis in range(3)]
            for i, item in posts(k, value > 0.0, value, vel, dirs, lambda i: f1[i, p - 1]).items():
                post[k, i, p - 1] = item

    def both(a, va, b, vb):
        return jnp.where(lane < 8, roll(a, -8 * va, 1), roll(b, 8 - 8 * vb, 1))

    value = [both(low, k, high, k) for k in range(2)]
    grad = []
    for k in range(2):
        a = jnp.abs(value[k])
        below = jnp.abs(both(low, 2 + k, own_high, k))
        above = jnp.abs(both(own_low, k, high, 2 + k))
        pz, w = above + below, above - below
        a_up, a_down = roll(a, -1, 0), roll(a, 1, 0)
        q = FACE * a + DIAG * (a_up + a_down + pz)
        v = a_up - a_down
        grad.append(
            (
                roll(q, -1, 1) - roll(q, 1, 1),
                FACE * v + DIAG * (roll(pz, -1, 0) - roll(pz, 1, 0) + roll(v, -1, 1) + roll(v, 1, 1)),
                FACE * w + DIAG * (roll(w, -1, 0) + roll(w, 1, 0) + roll(w, -1, 1) + roll(w, 1, 1)),
            )
        )
    sign = jnp.where(lane < 8, 1.0, -1.0)
    common = [both(low, 4 + axis, high, 4 + axis) for axis in range(3)]
    beyond = [
        posts(
            k,
            value[k] > 0.0,
            jnp.abs(value[k]),
            [sign * (common[axis] - (coupling * relax_times[k]) * grad[1 - k][axis]) for axis in range(3)],
            Z_LOW,
            lambda i: both(low, 7 + Z_LOW.index(i), high, 7 + Z_LOW.index(i)),
        )
        for k in range(2)
    ]

    for k in range(2):
        for i in range(19):
            cx, cy, cz = VELOCITIES[i]
            if cz:
                side = beyond[k][i if cz > 0 else OPPOSITE[i]]
                side = (roll(side, cy, 0) if cy else side)[0:16]
            for x in range(NX_L):
                fluid = flag[x] == 0
                old = f0[i, x] if k == 0 else f1[i, x + 1, 0:16, :]
                if i == 0:
                    moved = post[k, 0, x + 1, 0:16, :]
                else:
                    moved = post[k, i, x + 1 - cx]
                    moved = (roll(moved, cy, 0) if cy else moved)[0:16]
                    if cz > 0:
                        moved = jnp.where(lane16 == 0, roll(side, -(x - cx + 2), 1), roll(moved, 1, 1))
                    elif cz < 0:
                        moved = jnp.where(lane16 == 127, roll(side, 127 - (x - cx + 10), 1), roll(moved, -1, 1))
                    moved = jnp.where(moved < LIMIT, moved, post[k, OPPOSITE[i], x + 1, 0:16, :])
                out[k, i, x] = jnp.where(fluid, moved, old)

    for copy in copies.values():
        copy.wait_send()


def body(populations, solid):
    f32 = jnp.float32
    plane = (ROWS, NZ_L)
    scratch = [
        pltpu.VMEM((4, 16, 128), jnp.int32),
        pltpu.VMEM((19, 4, 16, 128), f32),
        pltpu.VMEM((19, 6, *plane), f32),
        pltpu.VMEM((2, 8, *plane), f32),
        pltpu.VMEM((3, 6, *plane), f32),
        *[pltpu.VMEM((2, 8, *plane), f32)] * 5,
        pltpu.VMEM((2, 19, 6, *plane), f32),
        *[pltpu.VMEM((2, 56, 128), f32)] * 2,
        *[pltpu.VMEM((2, 14, 16, 128), f32)] * 2,
        *[pltpu.VMEM((2, 2, 16, 128), f32)] * 2,
        pltpu.VMEM((2, 16, 128), f32),
        *[pltpu.VMEM((2, 8, 128), f32)] * 2,
        pltpu.VMEM((2, 2, 8, 128), f32),
        *[pltpu.VMEM((2, 2, 2, 128), f32)] * 2,
        pltpu.VMEM((2, 2, 2, 2, 128), f32),
        pltpu.VMEM((12, 8, 128), f32),
        pltpu.SemaphoreType.DMA((9,)),
        pltpu.SemaphoreType.DMA((26,)),
        pltpu.SemaphoreType.DMA((26,)),
        pltpu.SemaphoreType.REGULAR((26,)),
        pltpu.SemaphoreType.REGULAR,
    ]
    return pl.pallas_call(
        kernel,
        out_shape=jax.ShapeDtypeStruct(populations.shape, f32),
        in_specs=[pl.BlockSpec(memory_space=pltpu.HBM)] * 2,
        out_specs=pl.BlockSpec(memory_space=pltpu.VMEM),
        scratch_shapes=scratch,
        compiler_params=pltpu.CompilerParams(
            collective_id=0, has_side_effects=True, vmem_limit_bytes=40 * 1024 * 1024
        ),
    )(*[pltpu.with_memory_space_constraint(a, pltpu.HBM) for a in (populations, solid)])


def solution(mesh):
    in_specs = (P(None, None, "gx", "gy", "gz"), P("gx", "gy", "gz"))
    out_specs = P(None, None, "gx", "gy", "gz")
    return jax.shard_map(body, mesh=mesh, in_specs=in_specs, out_specs=out_specs, check_vma=False)
```

```python
import functools

import jax
import jax.numpy as jnp
from jax import lax
from jax.experimental import pallas as pl
from jax.experimental.pallas import tpu as pltpu
from jax.sharding import PartitionSpec as P

VELOCITIES = [
    (0, 0, 0),
    (1, 0, 0),
    (-1, 0, 0),
    (0, 1, 0),
    (0, -1, 0),
    (0, 0, 1),
    (0, 0, -1),
    (1, 1, 0),
    (-1, -1, 0),
    (1, -1, 0),
    (-1, 1, 0),
    (1, 0, 1),
    (-1, 0, -1),
    (1, 0, -1),
    (-1, 0, 1),
    (0, 1, 1),
    (0, -1, -1),
    (0, 1, -1),
    (0, -1, 1),
]
WEIGHTS = [1.0 / 3.0] + [1.0 / 18.0] * 6 + [1.0 / 36.0] * 12
OPPOSITE = [0, 2, 1, 4, 3, 6, 5, 8, 7, 10, 9, 12, 11, 14, 13, 16, 15, 18, 17]
PAIRS = [(1, 2), (3, 4), (5, 6), (7, 8), (9, 10), (11, 12), (13, 14), (15, 16), (17, 18)]
coupling = 0.9
relax_times = (1.0, 0.8)
wall_values = (0.3, 1.5)

NX_L, NY_L, NZ_L = 4, 16, 128
ROWS = 24
X_DIRS = ([i for i in range(19) if VELOCITIES[i][0] == 1], [i for i in range(19) if VELOCITIES[i][0] == -1])
Y_DIRS = ([i for i in range(19) if VELOCITIES[i][1] == 1], [i for i in range(19) if VELOCITIES[i][1] == -1])
Z_LOW = [i for i in range(19) if VELOCITIES[i][2] == 1]
Z_HIGH = [OPPOSITE[i] for i in Z_LOW]
BIG = 1e30
LIMIT = 1e28
FACE, DIAG = 1.0 / 18.0, 1.0 / 36.0
MESH = pl.DeviceIdType.MESH


def roll(a, shift, axis):
    return pltpu.roll(a, shift % a.shape[axis], axis)


def posts(k, fluid, rho, v, dirs, old):
    scale = 1.0 / relax_times[k]
    r = jnp.where(fluid, rho * scale, 0.0)
    b = [1.5 * c for c in v]
    quad = b[0] * b[0] + b[1] * b[1] + b[2] * b[2]
    base = r - (2.0 / 3.0) * r * quad
    base = jnp.where(fluid, base, BIG)
    out = {}

    def keep(i, eq):
        out[i] = eq if k == 0 else eq + (1.0 - scale) * old(i)

    if 0 in dirs:
        keep(0, WEIGHTS[0] * base)
    by_weight = {}
    for pair in PAIRS:
        if not any(i in dirs for i in pair):
            continue
        i = pair[0]
        w = WEIGHTS[i]
        if w not in by_weight:
            by_weight[w] = (w * base, (2.0 * w) * r)
        wb, wr = by_weight[w]
        along = None
        for axis in range(3):
            c = VELOCITIES[i][axis]
            if c:
                along = (b[axis] if c > 0 else -b[axis]) if along is None else (along + b[axis] if c > 0 else along - b[axis])
        t = wr * along
        s = wb + along * t
        if i in dirs:
            keep(i, s + t)
        if pair[1] in dirs:
            keep(pair[1], s - t)
    return out


def index_of(c):
    return 0 if c > 0 else 1


def ahead(ix, iz, nx, nz, dx, dz):
    if dz:
        rank = (lambda g: jnp.where(g < 2, g, 5 - g)) if nz == 4 else (lambda g: -g)
        return rank(iz) > rank(lax.rem(iz + dz + nz, nz))
    if dx:
        place = lambda g: jnp.where(lax.rem(g, 4) == 3, 1, 2 * lax.rem(g, 4))
        return place(ix) > place(lax.rem(ix + dx + nx, nx))
    return None


def vouched(ix, iz, nx, nz, dx, dz):
    if dx * dz >= 0:
        return jnp.bool_(False)
    return (ix == 0) & (iz == nz - 2) if dz > 0 else (ix == nx - 1) & (iz == nz - 1)


def kernel(
    pop, solid, out, flag, f0, f1, sp, u, gq, gvp, gv, gwp, gw, post,
    ys, yr, xs, xr, xys, xyr, tile, zs, zr, xzr, ps, yzr, xyzr, rest, sem_in, send, recv, go, vouch,
):
    ix, iy, iz = lax.axis_index("gx"), lax.axis_index("gy"), lax.axis_index("gz")
    nx, ny, nz = lax.axis_size("gx"), lax.axis_size("gy"), lax.axis_size("gz")
    around = (0, 1, -1)
    groups = [(dx, dz) for dz in (1, -1) for dx in around] + [(1, 0), (-1, 0)]
    leads = {g: ahead(ix, iz, nx, nz, *g) for g in groups}
    told = {g: vouched(ix, iz, nx, nz, *g) for g in groups}
    sends_first = {g: leads[g] & jnp.logical_not(told[g]) for g in groups}
    answers = {g: jnp.logical_not(leads[g] | told[g]) for g in groups}

    def target(dx, dy, dz):
        place = {}
        if dx:
            place["gx"] = lax.rem(ix + dx + nx, nx)
        if dy:
            place["gy"] = lax.rem(iy + dy + ny, ny)
        if dz:
            place["gz"] = lax.rem(iz + dz + nz, nz)
        return place

    mask_load = pltpu.make_async_copy(solid, flag, sem_in.at[8])
    loads = [
        (
            pltpu.make_async_copy(pop.at[0, :, x], f0.at[:, x], sem_in.at[2 * x]),
            pltpu.make_async_copy(pop.at[1, :, x], f1.at[:, x + 1, 0:16, :], sem_in.at[2 * x + 1]),
        )
        for x in range(NX_L)
    ]
    mask_load.start()
    for pair in loads:
        for copy in pair:
            copy.start()
    barrier = pltpu.get_barrier_semaphore()
    count = 2
    for dx, dz in groups:
        first = sends_first[dx, dz]
        count = count + 3 * first.astype(jnp.int32)

        @pl.when(answers[dx, dz])
        def _(dx=dx, dz=dz):
            for dy in around:
                pl.semaphore_signal(barrier, inc=1, device_id=target(dx, dy, dz), device_id_type=MESH)

    for dy in (1, -1):
        pl.semaphore_signal(barrier, inc=1, device_id=target(0, dy, 0), device_id_type=MESH)

    ways = [(dx, dy, dz) for dz in around for dx in around for dy in around if dx or dy or dz]
    copies = {}
    for n, (dx, dy, dz) in enumerate(ways):
        x, y, z = index_of(dx), index_of(dy), index_of(dz)
        if dz:
            src = ps.at[z, y] if dy else zs.at[z]
            if dx:
                dst = xyzr.at[x, y, z] if dy else xzr.at[x, z]
            else:
                dst = yzr.at[y, z] if dy else zr.at[z]
        elif dx:
            src, dst = (xys.at[x, y], xyr.at[x, y]) if dy else (xs.at[x], xr.at[x])
        else:
            src, dst = ys.at[y], yr.at[y]
        copies[dx, dy, dz] = pltpu.make_async_remote_copy(
            src_ref=src, dst_ref=dst, send_sem=send.at[n], recv_sem=recv.at[n],
            device_id=target(dx, dy, dz), device_id_type=MESH,
        )

    lane = lax.broadcasted_iota(jnp.int32, (ROWS, NZ_L), 1)
    lane16 = lax.broadcasted_iota(jnp.int32, (NY_L, NZ_L), 1)
    part = lax.broadcasted_iota(jnp.int32, (8, NZ_L), 1) % 8

    mask_load.wait()
    packed = [jnp.zeros((NY_L, NZ_L), jnp.float32) for s in range(2)]
    for x in range(NX_L):
        for copy in loads[x]:
            copy.wait()
        fluid = flag[x] == 0
        rho, momentum = [], []
        for k in range(2):
            f = (lambda i: f0[i, x]) if k == 0 else (lambda i: f1[i, x + 1, 0:16, :])
            total = f(0)
            mom = [None, None, None]
            for i, j in PAIRS:
                a, b = f(i), f(j)
                total = total + (a + b)
                d = a - b
                for axis in range(3):
                    c = VELOCITIES[i][axis]
                    if c:
                        mom[axis] = d * float(c) if mom[axis] is None else (mom[axis] + d if c > 0 else mom[axis] - d)
            rho.append(total)
            momentum.append(mom)
            sp[k, x + 2, 0:16, :] = jnp.where(fluid, total, -wall_values[k])
        inv = 1.0 / (rho[0] * (1.0 / relax_times[0]) + rho[1] * (1.0 / relax_times[1]))
        for axis in range(3):
            u[axis, x + 1, 0:16, :] = (
                momentum[0][axis] * (1.0 / relax_times[0]) + momentum[1][axis] * (1.0 / relax_times[1])
            ) * inv

        for s in range(2):
            near, far = ((127, 126), (0, 1))[s]
            dirs = (Z_LOW, Z_HIGH)[s]
            for v in range(12):
                if v < 4:
                    value, column = sp[v % 2, x + 2, 0:16, :], near if v < 2 else far
                elif v < 7:
                    value, column = u[v - 4, x + 1, 0:16, :], near
                else:
                    value, column = f1[dirs[v - 7], x + 1, 0:16, :], near
                spot = v * 8 + x + 2
                packed[s] = jnp.where(lane16 == spot, roll(value, spot - column, 1), packed[s])
    for s in range(2):
        tile[s] = packed[s]
        zs[s] = jnp.where((part >= 2) & (part <= 5), packed[s][0:8], roll(packed[s][8:16], 4, 1))
        ps[s, 0] = packed[s][14:16]
        ps[s, 1] = packed[s][0:2]

    def start_first(group):
        @pl.when(sends_first[group])
        def _():
            for dy in around:
                copies[group[0], dy, group[1]].start()

    def admit(group):
        @pl.when(sends_first[group])
        def _():
            for dy in around:
                way = (group[0], dy, group[1])
                pl.semaphore_signal(go.at[ways.index(way)], inc=1, device_id=target(*way), device_id_type=MESH)

    def answer(group):
        @pl.when(answers[group])
        def _():
            for dy in around:
                pl.semaphore_wait(go.at[ways.index((-group[0], -dy, -group[1]))], 1)
                copies[group[0], dy, group[1]].start()

    def collect(group):
        for dy in around:
            copies[-group[0], -dy, -group[1]].wait_recv()

    pl.semaphore_wait(barrier, count)
    for group in groups:
        admit(group)

    @pl.when((ix == nx - 1) & (iz == nz - 2))
    def _():
        pl.semaphore_signal(vouch, inc=1, device_id=target(1, 0, 0), device_id_type=MESH)
        pl.semaphore_signal(vouch, inc=1, device_id=target(0, 0, 1), device_id_type=MESH)
    for group in groups[:6]:
        start_first(group)

    for s in range(2):
        edge, two = ((15, 14), (0, 0))[s]
        for k in range(2):
            for x in range(NX_L):
                r = (k * 4 + x) * 2
                ys[s, r : r + 2, :] = sp[k, x + 2, two : two + 2, :]
        for axis in range(3):
            for x in range(NX_L):
                r = 16 + axis * 4 + x
                ys[s, r : r + 1, :] = u[axis, x + 1, edge : edge + 1, :]
        for j, i in enumerate(Y_DIRS[s]):
            for x in range(NX_L):
                r = 28 + j * 4 + x
                ys[s, r : r + 1, :] = f1[i, x + 1, edge : edge + 1, :]
        for side in range(2):
            ys[s, 48 + 2 * side : 50 + 2 * side, :] = tile[side, two : two + 2, :]
    for dy in (1, -1):
        copies[0, dy, 0].start()
    for s in range(2):
        last = 4 if s == 0 else 1
        planes = [(k, 2 + (2 + layer if s == 0 else layer)) for k in range(2) for layer in range(2)]
        for n, (k, plane) in enumerate(planes):
            xs[s, n] = sp[k, plane, 0:16, :]
        for axis in range(3):
            xs[s, 4 + axis] = u[axis, last, 0:16, :]
        for j, i in enumerate(X_DIRS[s]):
            xs[s, 7 + j] = f1[i, last, 0:16, :]
        for side in range(2):
            xs[s, 12 + side] = tile[side]
        for t in range(2):
            edge, two = ((15, 14), (0, 0))[t]
            for n, (k, plane) in enumerate(planes):
                xys[s, t, 2 * n : 2 * n + 2, :] = sp[k, plane, two : two + 2, :]
            for axis in range(3):
                xys[s, t, 8 + axis : 9 + axis, :] = u[axis, last, edge : edge + 1, :]
            i = VELOCITIES.index((1 - 2 * s, 1 - 2 * t, 0))
            xys[s, t, 11:12, :] = f1[i, last, edge : edge + 1, :]
            for side in range(2):
                xys[s, t, 12 + 2 * side : 14 + 2 * side, :] = tile[side, two : two + 2, :]
    for group in groups[6:]:
        start_first(group)
    def take_plane():
        for dy in (1, -1):
            copies[0, dy, 0].wait_recv()
        for group in groups[6:]:
            collect(group)
        for s in range(2):
            edge, two = ((23, 22), (16, 16))[s]
            for k in range(2):
                for x in range(NX_L):
                    r = (k * 4 + x) * 2
                    sp[k, x + 2, two : two + 2, :] = yr[s, r : r + 2, :]
            for axis in range(3):
                for x in range(NX_L):
                    r = 16 + axis * 4 + x
                    u[axis, x + 1, edge : edge + 1, :] = yr[s, r : r + 1, :]
            for j, i in enumerate(Y_DIRS[s]):
                for x in range(NX_L):
                    r = 28 + j * 4 + x
                    f1[i, x + 1, edge : edge + 1, :] = yr[s, r : r + 1, :]
        for s in range(2):
            last = 0 if s == 0 else 5
            planes = [(k, layer if s == 0 else 6 + layer) for k in range(2) for layer in range(2)]
            for n, (k, plane) in enumerate(planes):
                sp[k, plane, 0:16, :] = xr[s, n]
            for axis in range(3):
                u[axis, last, 0:16, :] = xr[s, 4 + axis]
            for j, i in enumerate(X_DIRS[s]):
                f1[i, last, 0:16, :] = xr[s, 7 + j]
            for t in range(2):
                edge, two = ((23, 22), (16, 16))[t]
                for n, (k, plane) in enumerate(planes):
                    sp[k, plane, two : two + 2, :] = xyr[s, t, 2 * n : 2 * n + 2, :]
                for axis in range(3):
                    u[axis, last, edge : edge + 1, :] = xyr[s, t, 8 + axis : 9 + axis, :]
                i = VELOCITIES.index((1 - 2 * s, 1 - 2 * t, 0))
                f1[i, last, edge : edge + 1, :] = xyr[s, t, 11:12, :]

    for group in groups[6:]:
        answer(group)
    for group in groups[:6]:
        answer(group)
    for group in ((1, -1), (-1, 1)):

        @pl.when(told[group])
        def _(group=group):
            pl.semaphore_wait(vouch, 1)
            for dy in around:
                copies[group[0], dy, group[1]].start()

    take_plane()
    for group in groups[:6]:
        collect(group)

    def merged(own, below, above):
        return jnp.where(part < 2, below, jnp.where(part > 5, above, own))

    def row_tile(n, after, before):
        rest[n, 6:8, :] = before
        rest[n, 0:2, :] = after
        return rest[n]

    def beyond_z(side):
        own, a, b = zr[side], xzr[0, side], xzr[1, side]
        n = side * 3
        third = merged(
            row_tile(n, yzr[1, side], yzr[0, side]),
            roll(row_tile(n + 1, xyzr[0, 1, side], xyzr[0, 0, side]), -4, 1),
            roll(row_tile(n + 2, xyzr[1, 1, side], xyzr[1, 0, side]), 4, 1),
        )
        return jnp.concatenate(
            [merged(own, roll(a, -4, 1), roll(b, 4, 1)), merged(roll(own, -4, 1), roll(a, -8, 1), b), third], axis=0
        )

    def own_z(side):
        n = 6 + side * 3
        r, q = slice(48 + 2 * side, 50 + 2 * side), slice(12 + 2 * side, 14 + 2 * side)
        third = merged(
            row_tile(n, yr[1, r, :], yr[0, r, :]),
            roll(row_tile(n + 1, xyr[0, 1, q, :], xyr[0, 0, q, :]), -4, 1),
            roll(row_tile(n + 2, xyr[1, 1, q, :], xyr[1, 0, q, :]), 4, 1),
        )
        rows = [
            merged(tile[side, h, :], roll(xr[0, 12 + side, h, :], -4, 1), roll(xr[1, 12 + side, h, :], 4, 1))
            for h in (slice(0, 8), slice(8, 16))
        ]
        return jnp.concatenate([*rows, third], axis=0)

    low, high = beyond_z(0), beyond_z(1)
    own_high, own_low = own_z(0), own_z(1)

    for k in range(2):
        for p in range(8):
            a = jnp.abs(sp[k, p])
            above = jnp.where(lane == 127, roll(jnp.abs(high), 127 - (k * 8 + p), 1), roll(a, -1, 1))
            below = jnp.where(lane == 0, roll(jnp.abs(low), -(k * 8 + p), 1), roll(a, 1, 1))
            pz, w = above + below, above - below
            a_up, a_down = roll(a, -1, 0), roll(a, 1, 0)
            gq[k, p] = FACE * a + DIAG * (a_up + a_down + pz)
            v = a_up - a_down
            gv[k, p] = DIAG * v
            gw[k, p] = DIAG * w
            if 1 <= p <= 6:
                gvp[k, p] = FACE * v + DIAG * (roll(pz, -1, 0) - roll(pz, 1, 0))
                gwp[k, p] = FACE * w + DIAG * (roll(w, -1, 0) + roll(w, 1, 0))

    for p in range(1, 7):
        grad = [
            (
                gq[k, p + 1] - gq[k, p - 1],
                gvp[k, p] + gv[k, p + 1] + gv[k, p - 1],
                gwp[k, p] + gw[k, p + 1] + gw[k, p - 1],
            )
            for k in range(2)
        ]
        dirs = X_DIRS[0] if p == 1 else X_DIRS[1] if p == 6 else list(range(19))
        for k in range(2):
            value = sp[k, p]
            vel = [u[axis, p - 1] - (coupling * relax_times[k]) * grad[1 - k][axis] for axis in range(3)]
            for i, item in posts(k, value > 0.0, value, vel, dirs, lambda i: f1[i, p - 1]).items():
                post[k, i, p - 1] = item

    def both(a, va, b, vb):
        return jnp.where(lane < 8, roll(a, -8 * va, 1), roll(b, 8 - 8 * vb, 1))

    value = [both(low, k, high, k) for k in range(2)]
    grad = []
    for k in range(2):
        a = jnp.abs(value[k])
        below = jnp.abs(both(low, 2 + k, own_high, k))
        above = jnp.abs(both(own_low, k, high, 2 + k))
        pz, w = above + below, above - below
        a_up, a_down = roll(a, -1, 0), roll(a, 1, 0)
        q = FACE * a + DIAG * (a_up + a_down + pz)
        v = a_up - a_down
        grad.append(
            (
                roll(q, -1, 1) - roll(q, 1, 1),
                FACE * v + DIAG * (roll(pz, -1, 0) - roll(pz, 1, 0) + roll(v, -1, 1) + roll(v, 1, 1)),
                FACE * w + DIAG * (roll(w, -1, 0) + roll(w, 1, 0) + roll(w, -1, 1) + roll(w, 1, 1)),
            )
        )
    sign = jnp.where(lane < 8, 1.0, -1.0)
    common = [both(low, 4 + axis, high, 4 + axis) for axis in range(3)]
    beyond = [
        posts(
            k,
            value[k] > 0.0,
            jnp.abs(value[k]),
            [sign * (common[axis] - (coupling * relax_times[k]) * grad[1 - k][axis]) for axis in range(3)],
            Z_LOW,
            lambda i: both(low, 7 + Z_LOW.index(i), high, 7 + Z_LOW.index(i)),
        )
        for k in range(2)
    ]

    for k in range(2):
        for i in range(19):
            cx, cy, cz = VELOCITIES[i]
            if cz:
                side = beyond[k][i if cz > 0 else OPPOSITE[i]]
                side = (roll(side, cy, 0) if cy else side)[0:16]
            for x in range(NX_L):
                fluid = flag[x] == 0
                old = f0[i, x] if k == 0 else f1[i, x + 1, 0:16, :]
                if i == 0:
                    moved = post[k, 0, x + 1, 0:16, :]
                else:
                    moved = post[k, i, x + 1 - cx]
                    moved = (roll(moved, cy, 0) if cy else moved)[0:16]
                    if cz > 0:
                        moved = jnp.where(lane16 == 0, roll(side, -(x - cx + 2), 1), roll(moved, 1, 1))
                    elif cz < 0:
                        moved = jnp.where(lane16 == 127, roll(side, 127 - (x - cx + 10), 1), roll(moved, -1, 1))
                    moved = jnp.where(moved < LIMIT, moved, post[k, OPPOSITE[i], x + 1, 0:16, :])
                out[k, i, x] = jnp.where(fluid, moved, old)

    for copy in copies.values():
        copy.wait_send()


def body(populations, solid):
    f32 = jnp.float32
    plane = (ROWS, NZ_L)
    scratch = [
        pltpu.VMEM((4, 16, 128), jnp.int32),
        pltpu.VMEM((19, 4, 16, 128), f32),
        pltpu.VMEM((19, 6, *plane), f32),
        pltpu.VMEM((2, 8, *plane), f32),
        pltpu.VMEM((3, 6, *plane), f32),
        *[pltpu.VMEM((2, 8, *plane), f32)] * 5,
        pltpu.VMEM((2, 19, 6, *plane), f32),
        *[pltpu.VMEM((2, 56, 128), f32)] * 2,
        *[pltpu.VMEM((2, 14, 16, 128), f32)] * 2,
        *[pltpu.VMEM((2, 2, 16, 128), f32)] * 2,
        pltpu.VMEM((2, 16, 128), f32),
        *[pltpu.VMEM((2, 8, 128), f32)] * 2,
        pltpu.VMEM((2, 2, 8, 128), f32),
        *[pltpu.VMEM((2, 2, 2, 128), f32)] * 2,
        pltpu.VMEM((2, 2, 2, 2, 128), f32),
        pltpu.VMEM((12, 8, 128), f32),
        pltpu.SemaphoreType.DMA((9,)),
        pltpu.SemaphoreType.DMA((26,)),
        pltpu.SemaphoreType.DMA((26,)),
        pltpu.SemaphoreType.REGULAR((26,)),
        pltpu.SemaphoreType.REGULAR,
    ]
    return pl.pallas_call(
        kernel,
        out_shape=jax.ShapeDtypeStruct(populations.shape, f32),
        in_specs=[pl.BlockSpec(memory_space=pltpu.HBM)] * 2,
        out_specs=pl.BlockSpec(memory_space=pltpu.VMEM),
        scratch_shapes=scratch,
        compiler_params=pltpu.CompilerParams(
            collective_id=0, has_side_effects=True, vmem_limit_bytes=40 * 1024 * 1024
        ),
    )(*[pltpu.with_memory_space_constraint(a, pltpu.HBM) for a in (populations, solid)])


def solution(mesh):
    in_specs = (P(None, None, "gx", "gy", "gz"), P("gx", "gy", "gz"))
    out_specs = P(None, None, "gx", "gy", "gz")
    return jax.shard_map(body, mesh=mesh, in_specs=in_specs, out_specs=out_specs, check_vma=False)
```

```python
import functools

import jax
import jax.numpy as jnp
from jax import lax
from jax.experimental import pallas as pl
from jax.experimental.pallas import tpu as pltpu
from jax.sharding import PartitionSpec as P

VELOCITIES = [
    (0, 0, 0),
    (1, 0, 0),
    (-1, 0, 0),
    (0, 1, 0),
    (0, -1, 0),
    (0, 0, 1),
    (0, 0, -1),
    (1, 1, 0),
    (-1, -1, 0),
    (1, -1, 0),
    (-1, 1, 0),
    (1, 0, 1),
    (-1, 0, -1),
    (1, 0, -1),
    (-1, 0, 1),
    (0, 1, 1),
    (0, -1, -1),
    (0, 1, -1),
    (0, -1, 1),
]
WEIGHTS = [1.0 / 3.0] + [1.0 / 18.0] * 6 + [1.0 / 36.0] * 12
OPPOSITE = [0, 2, 1, 4, 3, 6, 5, 8, 7, 10, 9, 12, 11, 14, 13, 16, 15, 18, 17]
PAIRS = [(1, 2), (3, 4), (5, 6), (7, 8), (9, 10), (11, 12), (13, 14), (15, 16), (17, 18)]
coupling = 0.9
relax_times = (1.0, 0.8)
wall_values = (0.3, 1.5)

NX_L, NY_L, NZ_L = 4, 16, 128
ROWS = 24
X_DIRS = ([i for i in range(19) if VELOCITIES[i][0] == 1], [i for i in range(19) if VELOCITIES[i][0] == -1])
Y_DIRS = ([i for i in range(19) if VELOCITIES[i][1] == 1], [i for i in range(19) if VELOCITIES[i][1] == -1])
Z_LOW = [i for i in range(19) if VELOCITIES[i][2] == 1]
Z_HIGH = [OPPOSITE[i] for i in Z_LOW]
BIG = 1e30
LIMIT = 1e28
FACE, DIAG = 1.0 / 18.0, 1.0 / 36.0
MESH = pl.DeviceIdType.MESH


def roll(a, shift, axis):
    return pltpu.roll(a, shift % a.shape[axis], axis)


def posts(k, fluid, rho, v, dirs, old):
    scale = 1.0 / relax_times[k]
    r = jnp.where(fluid, rho * scale, 0.0)
    b = [1.5 * c for c in v]
    quad = b[0] * b[0] + b[1] * b[1] + b[2] * b[2]
    base = r - (2.0 / 3.0) * r * quad
    base = jnp.where(fluid, base, BIG)
    out = {}

    def keep(i, eq):
        out[i] = eq if k == 0 else eq + (1.0 - scale) * old(i)

    if 0 in dirs:
        keep(0, WEIGHTS[0] * base)
    by_weight = {}
    for pair in PAIRS:
        if not any(i in dirs for i in pair):
            continue
        i = pair[0]
        w = WEIGHTS[i]
        if w not in by_weight:
            by_weight[w] = (w * base, (2.0 * w) * r)
        wb, wr = by_weight[w]
        along = None
        for axis in range(3):
            c = VELOCITIES[i][axis]
            if c:
                along = (b[axis] if c > 0 else -b[axis]) if along is None else (along + b[axis] if c > 0 else along - b[axis])
        t = wr * along
        s = wb + along * t
        if i in dirs:
            keep(i, s + t)
        if pair[1] in dirs:
            keep(pair[1], s - t)
    return out


def index_of(c):
    return 0 if c > 0 else 1


def ahead(ix, iz, nx, nz, dx, dz):
    if dz:
        rank = (lambda g: jnp.where(g < 2, g, 5 - g)) if nz == 4 else (lambda g: -g)
        return rank(iz) > rank(lax.rem(iz + dz + nz, nz))
    if dx:
        place = lambda g: jnp.where(lax.rem(g, 4) == 3, 1, 2 * lax.rem(g, 4))
        return place(ix) > place(lax.rem(ix + dx + nx, nx))
    return None


def vouched(ix, iz, nx, nz, dx, dz):
    if dx * dz >= 0:
        return jnp.bool_(False)
    return (ix == 0) & (iz == nz - 2) if dz > 0 else (ix == nx - 1) & (iz == nz - 1)


def kernel(
    pop, solid, out, flag, f0, f1, sp, u, gq, gvp, gv, gwp, gw, post,
    ys, yr, xs, xr, xys, xyr, tile, zs, zr, xzr, ps, yzr, xyzr, rest, sem_in, send, recv, go, vouch,
):
    ix, iy, iz = lax.axis_index("gx"), lax.axis_index("gy"), lax.axis_index("gz")
    nx, ny, nz = lax.axis_size("gx"), lax.axis_size("gy"), lax.axis_size("gz")
    around = (0, 1, -1)
    groups = [(dx, dz) for dz in (1, -1) for dx in (1, -1, 0)] + [(1, 0), (-1, 0)]
    leads = {g: ahead(ix, iz, nx, nz, *g) for g in groups}
    told = {g: vouched(ix, iz, nx, nz, *g) for g in groups}
    sends_first = {g: leads[g] & jnp.logical_not(told[g]) for g in groups}
    answers = {g: jnp.logical_not(leads[g] | told[g]) for g in groups}

    def target(dx, dy, dz):
        place = {}
        if dx:
            place["gx"] = lax.rem(ix + dx + nx, nx)
        if dy:
            place["gy"] = lax.rem(iy + dy + ny, ny)
        if dz:
            place["gz"] = lax.rem(iz + dz + nz, nz)
        return place

    mask_load = pltpu.make_async_copy(solid, flag, sem_in.at[8])
    loads = [
        (
            pltpu.make_async_copy(pop.at[0, :, x], f0.at[:, x], sem_in.at[2 * x]),
            pltpu.make_async_copy(pop.at[1, :, x], f1.at[:, x + 1, 0:16, :], sem_in.at[2 * x + 1]),
        )
        for x in range(NX_L)
    ]
    mask_load.start()
    for pair in loads:
        for copy in pair:
            copy.start()
    barrier = pltpu.get_barrier_semaphore()
    count = 2
    for dx, dz in groups:
        first = sends_first[dx, dz]
        count = count + 3 * first.astype(jnp.int32)

        @pl.when(answers[dx, dz])
        def _(dx=dx, dz=dz):
            for dy in around:
                pl.semaphore_signal(barrier, inc=1, device_id=target(dx, dy, dz), device_id_type=MESH)

    for dy in (1, -1):
        pl.semaphore_signal(barrier, inc=1, device_id=target(0, dy, 0), device_id_type=MESH)

    ways = [(dx, dy, dz) for dz in around for dx in around for dy in around if dx or dy or dz]
    copies = {}
    for n, (dx, dy, dz) in enumerate(ways):
        x, y, z = index_of(dx), index_of(dy), index_of(dz)
        if dz:
            src = ps.at[z, y] if dy else zs.at[z]
            if dx:
                dst = xyzr.at[x, y, z] if dy else xzr.at[x, z]
            else:
                dst = yzr.at[y, z] if dy else zr.at[z]
        elif dx:
            src, dst = (xys.at[x, y], xyr.at[x, y]) if dy else (xs.at[x], xr.at[x])
        else:
            src, dst = ys.at[y], yr.at[y]
        copies[dx, dy, dz] = pltpu.make_async_remote_copy(
            src_ref=src, dst_ref=dst, send_sem=send.at[n], recv_sem=recv.at[n],
            device_id=target(dx, dy, dz), device_id_type=MESH,
        )

    lane = lax.broadcasted_iota(jnp.int32, (ROWS, NZ_L), 1)
    lane16 = lax.broadcasted_iota(jnp.int32, (NY_L, NZ_L), 1)
    part = lax.broadcasted_iota(jnp.int32, (8, NZ_L), 1) % 8

    mask_load.wait()
    packed = [jnp.zeros((NY_L, NZ_L), jnp.float32) for s in range(2)]
    for x in range(NX_L):
        for copy in loads[x]:
            copy.wait()
        fluid = flag[x] == 0
        rho, momentum = [], []
        for k in range(2):
            f = (lambda i: f0[i, x]) if k == 0 else (lambda i: f1[i, x + 1, 0:16, :])
            total = f(0)
            mom = [None, None, None]
            for i, j in PAIRS:
                a, b = f(i), f(j)
                total = total + (a + b)
                d = a - b
                for axis in range(3):
                    c = VELOCITIES[i][axis]
                    if c:
                        mom[axis] = d * float(c) if mom[axis] is None else (mom[axis] + d if c > 0 else mom[axis] - d)
            rho.append(total)
            momentum.append(mom)
            sp[k, x + 2, 0:16, :] = jnp.where(fluid, total, -wall_values[k])
        inv = 1.0 / (rho[0] * (1.0 / relax_times[0]) + rho[1] * (1.0 / relax_times[1]))
        for axis in range(3):
            u[axis, x + 1, 0:16, :] = (
                momentum[0][axis] * (1.0 / relax_times[0]) + momentum[1][axis] * (1.0 / relax_times[1])
            ) * inv

        for s in range(2):
            near, far = ((127, 126), (0, 1))[s]
            dirs = (Z_LOW, Z_HIGH)[s]
            for v in range(12):
                if v < 4:
                    value, column = sp[v % 2, x + 2, 0:16, :], near if v < 2 else far
                elif v < 7:
                    value, column = u[v - 4, x + 1, 0:16, :], near
                else:
                    value, column = f1[dirs[v - 7], x + 1, 0:16, :], near
                spot = v * 8 + x + 2
                packed[s] = jnp.where(lane16 == spot, roll(value, spot - column, 1), packed[s])
    for s in range(2):
        tile[s] = packed[s]
        zs[s] = jnp.where((part >= 2) & (part <= 5), packed[s][0:8], roll(packed[s][8:16], 4, 1))
        ps[s, 0] = packed[s][14:16]
        ps[s, 1] = packed[s][0:2]

    def start_first(group):
        @pl.when(sends_first[group])
        def _():
            for dy in around:
                copies[group[0], dy, group[1]].start()

    def admit(group):
        @pl.when(sends_first[group])
        def _():
            for dy in around:
                way = (group[0], dy, group[1])
                pl.semaphore_signal(go.at[ways.index(way)], inc=1, device_id=target(*way), device_id_type=MESH)

    def answer(group):
        @pl.when(answers[group])
        def _():
            for dy in around:
                pl.semaphore_wait(go.at[ways.index((-group[0], -dy, -group[1]))], 1)
                copies[group[0], dy, group[1]].start()

    def collect(group):
        for dy in around:
            copies[-group[0], -dy, -group[1]].wait_recv()

    pl.semaphore_wait(barrier, count)
    for group in groups:
        admit(group)

    @pl.when((ix == nx - 1) & (iz == nz - 2))
    def _():
        pl.semaphore_signal(vouch, inc=1, device_id=target(1, 0, 0), device_id_type=MESH)
        pl.semaphore_signal(vouch, inc=1, device_id=target(0, 0, 1), device_id_type=MESH)
    for group in groups[:6]:
        start_first(group)

    for s in range(2):
        edge, two = ((15, 14), (0, 0))[s]
        for k in range(2):
            for x in range(NX_L):
                r = (k * 4 + x) * 2
                ys[s, r : r + 2, :] = sp[k, x + 2, two : two + 2, :]
        for axis in range(3):
            for x in range(NX_L):
                r = 16 + axis * 4 + x
                ys[s, r : r + 1, :] = u[axis, x + 1, edge : edge + 1, :]
        for j, i in enumerate(Y_DIRS[s]):
            for x in range(NX_L):
                r = 28 + j * 4 + x
                ys[s, r : r + 1, :] = f1[i, x + 1, edge : edge + 1, :]
        for side in range(2):
            ys[s, 48 + 2 * side : 50 + 2 * side, :] = tile[side, two : two + 2, :]
    for dy in (1, -1):
        copies[0, dy, 0].start()
    for s in range(2):
        last = 4 if s == 0 else 1
        planes = [(k, 2 + (2 + layer if s == 0 else layer)) for k in range(2) for layer in range(2)]
        for n, (k, plane) in enumerate(planes):
            xs[s, n] = sp[k, plane, 0:16, :]
        for axis in range(3):
            xs[s, 4 + axis] = u[axis, last, 0:16, :]
        for j, i in enumerate(X_DIRS[s]):
            xs[s, 7 + j] = f1[i, last, 0:16, :]
        for side in range(2):
            xs[s, 12 + side] = tile[side]
        for t in range(2):
            edge, two = ((15, 14), (0, 0))[t]
            for n, (k, plane) in enumerate(planes):
                xys[s, t, 2 * n : 2 * n + 2, :] = sp[k, plane, two : two + 2, :]
            for axis in range(3):
                xys[s, t, 8 + axis : 9 + axis, :] = u[axis, last, edge : edge + 1, :]
            i = VELOCITIES.index((1 - 2 * s, 1 - 2 * t, 0))
            xys[s, t, 11:12, :] = f1[i, last, edge : edge + 1, :]
            for side in range(2):
                xys[s, t, 12 + 2 * side : 14 + 2 * side, :] = tile[side, two : two + 2, :]
    for group in groups[6:]:
        start_first(group)
    def take_plane():
        for dy in (1, -1):
            copies[0, dy, 0].wait_recv()
        for group in groups[6:]:
            collect(group)
        for s in range(2):
            edge, two = ((23, 22), (16, 16))[s]
            for k in range(2):
                for x in range(NX_L):
                    r = (k * 4 + x) * 2
                    sp[k, x + 2, two : two + 2, :] = yr[s, r : r + 2, :]
            for axis in range(3):
                for x in range(NX_L):
                    r = 16 + axis * 4 + x
                    u[axis, x + 1, edge : edge + 1, :] = yr[s, r : r + 1, :]
            for j, i in enumerate(Y_DIRS[s]):
                for x in range(NX_L):
                    r = 28 + j * 4 + x
                    f1[i, x + 1, edge : edge + 1, :] = yr[s, r : r + 1, :]
        for s in range(2):
            last = 0 if s == 0 else 5
            planes = [(k, layer if s == 0 else 6 + layer) for k in range(2) for layer in range(2)]
            for n, (k, plane) in enumerate(planes):
                sp[k, plane, 0:16, :] = xr[s, n]
            for axis in range(3):
                u[axis, last, 0:16, :] = xr[s, 4 + axis]
            for j, i in enumerate(X_DIRS[s]):
                f1[i, last, 0:16, :] = xr[s, 7 + j]
            for t in range(2):
                edge, two = ((23, 22), (16, 16))[t]
                for n, (k, plane) in enumerate(planes):
                    sp[k, plane, two : two + 2, :] = xyr[s, t, 2 * n : 2 * n + 2, :]
                for axis in range(3):
                    u[axis, last, edge : edge + 1, :] = xyr[s, t, 8 + axis : 9 + axis, :]
                i = VELOCITIES.index((1 - 2 * s, 1 - 2 * t, 0))
                f1[i, last, edge : edge + 1, :] = xyr[s, t, 11:12, :]

    for group in groups[6:]:
        answer(group)
    for group in groups[:6]:
        answer(group)
    for group in ((1, -1), (-1, 1)):

        @pl.when(told[group])
        def _(group=group):
            pl.semaphore_wait(vouch, 1)
            for dy in around:
                copies[group[0], dy, group[1]].start()

    take_plane()
    for group in groups[:6]:
        collect(group)

    def merged(own, below, above):
        return jnp.where(part < 2, below, jnp.where(part > 5, above, own))

    def row_tile(n, after, before):
        rest[n, 6:8, :] = before
        rest[n, 0:2, :] = after
        return rest[n]

    def beyond_z(side):
        own, a, b = zr[side], xzr[0, side], xzr[1, side]
        n = side * 3
        third = merged(
            row_tile(n, yzr[1, side], yzr[0, side]),
            roll(row_tile(n + 1, xyzr[0, 1, side], xyzr[0, 0, side]), -4, 1),
            roll(row_tile(n + 2, xyzr[1, 1, side], xyzr[1, 0, side]), 4, 1),
        )
        return jnp.concatenate(
            [merged(own, roll(a, -4, 1), roll(b, 4, 1)), merged(roll(own, -4, 1), roll(a, -8, 1), b), third], axis=0
        )

    def own_z(side):
        n = 6 + side * 3
        r, q = slice(48 + 2 * side, 50 + 2 * side), slice(12 + 2 * side, 14 + 2 * side)
        third = merged(
            row_tile(n, yr[1, r, :], yr[0, r, :]),
            roll(row_tile(n + 1, xyr[0, 1, q, :], xyr[0, 0, q, :]), -4, 1),
            roll(row_tile(n + 2, xyr[1, 1, q, :], xyr[1, 0, q, :]), 4, 1),
        )
        rows = [
            merged(tile[side, h, :], roll(xr[0, 12 + side, h, :], -4, 1), roll(xr[1, 12 + side, h, :], 4, 1))
            for h in (slice(0, 8), slice(8, 16))
        ]
        return jnp.concatenate([*rows, third], axis=0)

    low, high = beyond_z(0), beyond_z(1)
    own_high, own_low = own_z(0), own_z(1)

    for k in range(2):
        for p in range(8):
            a = jnp.abs(sp[k, p])
            above = jnp.where(lane == 127, roll(jnp.abs(high), 127 - (k * 8 + p), 1), roll(a, -1, 1))
            below = jnp.where(lane == 0, roll(jnp.abs(low), -(k * 8 + p), 1), roll(a, 1, 1))
            pz, w = above + below, above - below
            a_up, a_down = roll(a, -1, 0), roll(a, 1, 0)
            gq[k, p] = FACE * a + DIAG * (a_up + a_down + pz)
            v = a_up - a_down
            gv[k, p] = DIAG * v
            gw[k, p] = DIAG * w
            if 1 <= p <= 6:
                gvp[k, p] = FACE * v + DIAG * (roll(pz, -1, 0) - roll(pz, 1, 0))
                gwp[k, p] = FACE * w + DIAG * (roll(w, -1, 0) + roll(w, 1, 0))

    for p in range(1, 7):
        grad = [
            (
                gq[k, p + 1] - gq[k, p - 1],
                gvp[k, p] + gv[k, p + 1] + gv[k, p - 1],
                gwp[k, p] + gw[k, p + 1] + gw[k, p - 1],
            )
            for k in range(2)
        ]
        dirs = X_DIRS[0] if p == 1 else X_DIRS[1] if p == 6 else list(range(19))
        for k in range(2):
            value = sp[k, p]
            vel = [u[axis, p - 1] - (coupling * relax_times[k]) * grad[1 - k][axis] for axis in range(3)]
            for i, item in posts(k, value > 0.0, value, vel, dirs, lambda i: f1[i, p - 1]).items():
                post[k, i, p - 1] = item

    def both(a, va, b, vb):
        return jnp.where(lane < 8, roll(a, -8 * va, 1), roll(b, 8 - 8 * vb, 1))

    value = [both(low, k, high, k) for k in range(2)]
    grad = []
    for k in range(2):
        a = jnp.abs(value[k])
        below = jnp.abs(both(low, 2 + k, own_high, k))
        above = jnp.abs(both(own_low, k, high, 2 + k))
        pz, w = above + below, above - below
        a_up, a_down = roll(a, -1, 0), roll(a, 1, 0)
        q = FACE * a + DIAG * (a_up + a_down + pz)
        v = a_up - a_down
        grad.append(
            (
                roll(q, -1, 1) - roll(q, 1, 1),
                FACE * v + DIAG * (roll(pz, -1, 0) - roll(pz, 1, 0) + roll(v, -1, 1) + roll(v, 1, 1)),
                FACE * w + DIAG * (roll(w, -1, 0) + roll(w, 1, 0) + roll(w, -1, 1) + roll(w, 1, 1)),
            )
        )
    sign = jnp.where(lane < 8, 1.0, -1.0)
    common = [both(low, 4 + axis, high, 4 + axis) for axis in range(3)]
    beyond = [
        posts(
            k,
            value[k] > 0.0,
            jnp.abs(value[k]),
            [sign * (common[axis] - (coupling * relax_times[k]) * grad[1 - k][axis]) for axis in range(3)],
            Z_LOW,
            lambda i: both(low, 7 + Z_LOW.index(i), high, 7 + Z_LOW.index(i)),
        )
        for k in range(2)
    ]

    for k in range(2):
        for i in range(19):
            cx, cy, cz = VELOCITIES[i]
            if cz:
                side = beyond[k][i if cz > 0 else OPPOSITE[i]]
                side = (roll(side, cy, 0) if cy else side)[0:16]
            for x in range(NX_L):
                fluid = flag[x] == 0
                old = f0[i, x] if k == 0 else f1[i, x + 1, 0:16, :]
                if i == 0:
                    moved = post[k, 0, x + 1, 0:16, :]
                else:
                    moved = post[k, i, x + 1 - cx]
                    moved = (roll(moved, cy, 0) if cy else moved)[0:16]
                    if cz > 0:
                        moved = jnp.where(lane16 == 0, roll(side, -(x - cx + 2), 1), roll(moved, 1, 1))
                    elif cz < 0:
                        moved = jnp.where(lane16 == 127, roll(side, 127 - (x - cx + 10), 1), roll(moved, -1, 1))
                    moved = jnp.where(moved < LIMIT, moved, post[k, OPPOSITE[i], x + 1, 0:16, :])
                out[k, i, x] = jnp.where(fluid, moved, old)

    for copy in copies.values():
        copy.wait_send()


def body(populations, solid):
    f32 = jnp.float32
    plane = (ROWS, NZ_L)
    scratch = [
        pltpu.VMEM((4, 16, 128), jnp.int32),
        pltpu.VMEM((19, 4, 16, 128), f32),
        pltpu.VMEM((19, 6, *plane), f32),
        pltpu.VMEM((2, 8, *plane), f32),
        pltpu.VMEM((3, 6, *plane), f32),
        *[pltpu.VMEM((2, 8, *plane), f32)] * 5,
        pltpu.VMEM((2, 19, 6, *plane), f32),
        *[pltpu.VMEM((2, 56, 128), f32)] * 2,
        *[pltpu.VMEM((2, 14, 16, 128), f32)] * 2,
        *[pltpu.VMEM((2, 2, 16, 128), f32)] * 2,
        pltpu.VMEM((2, 16, 128), f32),
        *[pltpu.VMEM((2, 8, 128), f32)] * 2,
        pltpu.VMEM((2, 2, 8, 128), f32),
        *[pltpu.VMEM((2, 2, 2, 128), f32)] * 2,
        pltpu.VMEM((2, 2, 2, 2, 128), f32),
        pltpu.VMEM((12, 8, 128), f32),
        pltpu.SemaphoreType.DMA((9,)),
        pltpu.SemaphoreType.DMA((26,)),
        pltpu.SemaphoreType.DMA((26,)),
        pltpu.SemaphoreType.REGULAR((26,)),
        pltpu.SemaphoreType.REGULAR,
    ]
    return pl.pallas_call(
        kernel,
        out_shape=jax.ShapeDtypeStruct(populations.shape, f32),
        in_specs=[pl.BlockSpec(memory_space=pltpu.HBM)] * 2,
        out_specs=pl.BlockSpec(memory_space=pltpu.VMEM),
        scratch_shapes=scratch,
        compiler_params=pltpu.CompilerParams(
            collective_id=0, has_side_effects=True, vmem_limit_bytes=40 * 1024 * 1024
        ),
    )(*[pltpu.with_memory_space_constraint(a, pltpu.HBM) for a in (populations, solid)])


def solution(mesh):
    in_specs = (P(None, None, "gx", "gy", "gz"), P("gx", "gy", "gz"))
    out_specs = P(None, None, "gx", "gy", "gz")
    return jax.shard_map(body, mesh=mesh, in_specs=in_specs, out_specs=out_specs, check_vma=False)
```
